32 devices in a mesh: dp: 4 (over y, x), expert: 8 (over z, core).
Axes of the slice: x: 2, y: 2, z: 4, core: 2. Of those that a mesh axis runs over, the one named last changes fastest.
Arguments:
- tokens: bfloat16 [4096, 4096], P(('dp', 'expert')), may hold values from -6 to 6
- routes: int32 [4096, 2], P(('dp', 'expert')), may hold values from 0 to 7, all different within a row; in each aligned block of 128 rows (0 to 127, 128 to 255, ...) at most 48 rows name the same one
- router_weight: bfloat16 [4096, 8], replicated, may hold values from -0.09375 to 0.09375
- shift: float32 [1, 4096], replicated, may hold values from -3 to 3
- scale: float32 [1, 4096], replicated, may hold values from -3 to 3
- gate_mod: float32 [1, 4096], replicated, may hold values from -4 to 4
- gate_weight: bfloat16 [8, 4096, 1024], P(None, ('dp', 'expert')), may hold values from -0.09375 to 0.09375
- up_weight: bfloat16 [8, 4096, 1024], P(None, ('dp', 'expert')), may hold values from -0.09375 to 0.09375
- down_weight: bfloat16 [8, 4096, 1024], P(None, ('dp', 'expert')), may hold values from -0.1875 to 0.1875
Outputs:
- update: bfloat16 [4096, 4096], P(('dp', 'expert'))
The draws below stay inside these ranges and needn't reach their ends.
Inputs may be any that keep to these rules, and one draw needn't show every extreme that they name: `routes`: each row names two different experts; among the rows of one device no expert is named more than 48 times, a bound that some block reaches.
All inputs are finite; a program needn't handle non-finite values.
Results may differ from the reference program's by a relative error of at most 0.0072.
Values may be sent and summed in bfloat16 or wider, within the bound.
No kernel may reach another device: no remote copies, remote signals or barrier semaphores. Data moves between devices by JAX's collectives and lax.ppermute only.
A program may use at most 128 MiB of HBM per device.

```python
import math
import jax
import jax.numpy as jnp
import numpy as np
from jax import lax

D = 4096
FE = 1024
E = 8
TOK_DEV = 128
CAP = 48
PIX = 4096
TOKENS = 4096
IMAGES = 1


def steps_of(key, extent, cuts, least, high):
    level, own = 1.0, jax.random.fold_in(key, 6)
    for dim, blocks in cuts:
        steps = jnp.exp(jax.random.uniform(jax.random.fold_in(own, dim), (blocks,), jnp.float32, least / len(cuts), high / len(cuts)))
        level = level * jnp.repeat(steps, extent[dim] // blocks).reshape([-1 if axis == dim else 1 for axis in range(len(extent))])
    return level


def routed_block(rng, own, number, rows, count, top, limit, skew):
    order = jax.random.permutation(rng, count)
    crowded, usual = shares(count, rows * top, limit, skew, True), shares(count, rows * top, limit, skew, False)
    places = jnp.arange(count)

    def named(tallies, turn):
        used = int((tallies > 0).sum())
        fixed = max(1, used // 4)
        moved = fixed + (places - fixed + turn * (used - fixed)) % max(1, count - fixed)
        return jnp.zeros((count,), jnp.int32).at[order[jnp.where(places < fixed, places, moved)]].set(jnp.asarray(tallies, jnp.int32))

    tallies = jnp.where(number % 4 == 0, named(crowded, number // 4), named(usual, number - number // 4 - 1))
    mixed = jax.random.permutation(jax.random.fold_in(own, 3), count)
    donor, receiver = mixed[0:count // 2 * 2:2], mixed[1:count // 2 * 2:2]
    margin = jnp.minimum(tallies[donor] - 1, limit - tallies[receiver]) // 2
    margin = jnp.where((donor == order[0]) | (receiver == order[0]) | (tallies[receiver] == 0), 0, jnp.maximum(margin, 0))
    moved = jax.random.randint(jax.random.fold_in(own, 4), (count // 2,), 0, 1 << 20) % (margin + 1)
    tallies = tallies.at[donor].add(-moved).at[receiver].add(moved)
    labels = jnp.searchsorted(jnp.cumsum(tallies), jnp.arange(rows * top), side="right").astype(jnp.int32)
    listing = labels.reshape(top, rows).T
    listing = listing[jax.random.permutation(jax.random.fold_in(own, 1), rows)]
    turn = jax.random.randint(jax.random.fold_in(own, 2), (rows, 1), 0, top)
    return jnp.take_along_axis(listing, (jnp.arange(top)[None, :] + turn) % top, axis=1)


def shares(number_of, total, reach, lean, full):
    loads = [(1 << 20) // math.isqrt(rank ** lean) + 1 for rank in range(1, number_of + 1)]
    largest = reach if full else min(reach, max(-(-total // number_of), total * loads[0] // sum(loads)))
    least = 1 if total - largest >= number_of - 1 else 0
    given, rest = [largest] + [least] * (number_of - 1), total - largest - least * (number_of - 1)
    while rest > 0:
        candidates = [i for i in range(1, number_of) if given[i] < largest] or [i for i in range(1, number_of) if given[i] < reach]
        mass, budget = sum([loads[i] for i in candidates]), rest
        for i in candidates:
            addition = min(reach - given[i], max(1, budget * loads[i] // mass), rest)
            given[i] = given[i] + addition
            rest = rest - addition
    return np.array(given)


def gaussian(rng, shape, scale, bound, pieces=(), kind=jnp.bfloat16):
    factor_of = steps_of(rng, shape, pieces, -0.22, 0.18) if pieces else 1.0
    result = jax.random.normal(rng, shape, jnp.float32) * scale * factor_of
    return jnp.minimum(jnp.maximum(result, -bound), bound).astype(kind)


def setup_inputs(seed: int = 0) -> dict:
    arg_keys = jax.random.split(jax.random.key(seed), 10)
    tokens = gaussian(arg_keys[0], (TOKENS, D), 1.0, 6.0, ((0, 32),))
    routes_keys = jax.random.split(jax.random.fold_in(arg_keys[1], 1), TOKENS // TOK_DEV)
    routes_turns = jax.random.permutation(jax.random.fold_in(arg_keys[1], 3), TOKENS // TOK_DEV)
    routes = jax.vmap(lambda own, number: routed_block(jax.random.fold_in(arg_keys[1], 2), own, number, TOK_DEV, E, 2, CAP, 2))(routes_keys, routes_turns).reshape((TOKENS, 2))
    router_weight = gaussian(arg_keys[2], (D, E), D ** -0.5, 0.09375)
    shift = gaussian(arg_keys[3], (IMAGES, D), 0.5, 3.0, (), jnp.float32)
    scale = gaussian(arg_keys[4], (IMAGES, D), 0.5, 3.0, (), jnp.float32)
    gate_mod = gaussian(arg_keys[5], (IMAGES, D), 1.0, 4.0, (), jnp.float32)
    gate_weight = gaussian(arg_keys[6], (E, D, FE), D ** -0.5, 0.09375, ((1, 32),))
    up_weight = gaussian(arg_keys[7], (E, D, FE), D ** -0.5, 0.09375, ((1, 32),))
    down_weight = gaussian(arg_keys[8], (E, D, FE), FE ** -0.5, 0.1875, ((1, 32),))
    return dict(tokens=tokens, routes=routes, router_weight=router_weight, shift=shift, scale=scale, gate_mod=gate_mod, gate_weight=gate_weight, up_weight=up_weight, down_weight=down_weight)


EPS = 1e-06

def reference(tokens, routes, router_weight, shift, scale, gate_mod, gate_weight, up_weight, down_weight):
    blocks = TOKENS // TOK_DEV

    def norm_image(items):
        rows, image_shift, image_scale = items
        values = rows.astype(jnp.float32)
        meansq = lax.optimization_barrier(jnp.mean(values * values, axis=-1, keepdims=True))
        normed_rows = values * lax.rsqrt(meansq + EPS) * (1.0 + image_scale[None, :]) + image_shift[None, :]
        normed_rows = normed_rows.astype(jnp.bfloat16)
        logit_rows = jnp.dot(normed_rows, router_weight, preferred_element_type=jnp.float32)
        return (normed_rows, logit_rows)
    normed, logits = lax.map(norm_image, (tokens.reshape(IMAGES, PIX, D), shift, scale))
    normed = normed.reshape(TOKENS, D)
    logits = logits.reshape(TOKENS, E)
    chosen = jnp.take_along_axis(logits, routes, axis=1)
    score_flat = jax.nn.sigmoid(chosen).reshape(-1)
    flat = routes.reshape(blocks, 2 * TOK_DEV)
    hot = (flat[:, :, None] == jnp.arange(E, dtype=jnp.int32)[None, None, :]).astype(jnp.int32)
    rank = (jnp.cumsum(hot, axis=1) - hot).astype(jnp.int32)
    slot = lax.optimization_barrier(jnp.sum(rank * hot, axis=-1)).astype(jnp.int32)
    position = (flat * CAP + slot).astype(jnp.int32)
    global_ids = (jnp.arange(blocks, dtype=jnp.int32)[:, None] * (2 * TOK_DEV) + jnp.arange(2 * TOK_DEV, dtype=jnp.int32)[None, :]).astype(jnp.int32)

    def fill_table(where_to, ids):
        return jnp.full((E * CAP,), -1, jnp.int32).at[where_to].set(ids)
    table = jax.vmap(fill_table)(position, global_ids)
    table = table.reshape(blocks, E, CAP).transpose(1, 0, 2).reshape(E, blocks * CAP)

    def expert_step(total, items):
        ids, w_gate, w_up, w_down = items
        filled = ids >= 0
        safe = jnp.where(filled, ids, 0).astype(jnp.int32)
        token_ids = (safe // 2).astype(jnp.int32)
        rows = jnp.where(filled[:, None], normed[token_ids], jnp.zeros((), jnp.bfloat16))
        gate = jnp.dot(rows, w_gate, preferred_element_type=jnp.float32)
        upper = jnp.dot(rows, w_up, preferred_element_type=jnp.float32)
        hidden = (jax.nn.silu(gate) * upper).astype(jnp.bfloat16)
        output = jnp.dot(hidden, w_down.T, preferred_element_type=jnp.float32).astype(jnp.bfloat16)
        weight = jnp.where(filled, score_flat[safe], jnp.zeros((), jnp.float32))
        total = total.at[token_ids].add(weight[:, None] * output.astype(jnp.float32))
        return (total, None)
    total, unused = lax.scan(expert_step, jnp.zeros((TOKENS, D), jnp.float32), (table, gate_weight, up_weight, down_weight))
    update = total.reshape(IMAGES, PIX, D) * gate_mod[:, None, :]
    return update.reshape(TOKENS, D).astype(jnp.bfloat16)
```

```python
import jax
import jax.numpy as jnp
from jax import lax
from jax.experimental import pallas as pl
from jax.experimental.pallas import tpu as pltpu
from jax.sharding import PartitionSpec as P

PIX = 4096
EPS = 1e-06
AXES = ("dp", "expert")


def gate_up_kernel(info_ref, x_ref, gate_a, gate_b, up_a, up_b, out_ref, acc_ref):
    e = pl.program_id(0)
    half = x_ref.shape[1] // 2
    hid = gate_a.shape[-1]
    xa, xb = x_ref[:, :half], x_ref[:, half:]

    def product(first, second):
        total = jnp.dot(xa, first[...].reshape(half, hid), preferred_element_type=jnp.float32)
        return total + jnp.dot(xb, second[...].reshape(half, hid), preferred_element_type=jnp.float32)

    gate = product(gate_a, gate_b)
    upper = product(up_a, up_b)
    mine = e.astype(jnp.float32)

    @pl.when(e == 0)
    def _():
        acc_ref[...] = jnp.zeros_like(acc_ref)

    for k in range(2):
        chosen = info_ref[:, k : k + 1] == mine
        base = 2 * hid * k
        acc_ref[:, base : base + hid] = jnp.where(chosen, gate, acc_ref[:, base : base + hid])
        acc_ref[:, base + hid : base + 2 * hid] = jnp.where(
            chosen, upper, acc_ref[:, base + hid : base + 2 * hid]
        )

    @pl.when(e == pl.num_programs(0) - 1)
    def _():
        out_ref[...] = acc_ref[...].astype(out_ref.dtype)


def gate_up(info, x, gate, up):
    experts, blocks, rows, hid = gate[0].shape
    tokens = x.shape[0]
    weight = pl.BlockSpec((1, blocks, rows, hid), lambda e: (e, 0, 0, 0))
    return pl.pallas_call(
        gate_up_kernel,
        grid=(experts,),
        in_specs=[
            pl.BlockSpec(info.shape, lambda e: (0, 0)),
            pl.BlockSpec(x.shape, lambda e: (0, 0)),
            weight,
            weight,
            weight,
            weight,
        ],
        out_specs=pl.BlockSpec((tokens, 4 * hid), lambda e: (0, 0)),
        out_shape=jax.ShapeDtypeStruct((tokens, 4 * hid), jnp.bfloat16),
        scratch_shapes=[pltpu.VMEM((tokens, 4 * hid), jnp.float32)],
        cost_estimate=pl.CostEstimate(
            flops=experts * 4 * tokens * x.shape[1] * hid, transcendentals=0, bytes_accessed=4 * gate[0].size * 2
        ),
        name="gate_up",
    )(info, x, gate[0], gate[1], up[0], up[1])


def down_kernel(info_ref, h_ref, down_a, down_b, out_ref, acc_ref):
    e = pl.program_id(0)
    hid = h_ref.shape[1] // 2
    half = out_ref.shape[1] // 2
    mine = e.astype(jnp.float32)
    zero = jnp.zeros((), jnp.bfloat16)
    first = jnp.where(info_ref[:, 0:1] == mine, h_ref[:, :hid], zero)
    h = jnp.where(info_ref[:, 1:2] == mine, h_ref[:, hid:], first)

    @pl.when(e == 0)
    def _():
        acc_ref[...] = jnp.zeros_like(acc_ref)

    for side, ref in enumerate((down_a, down_b)):
        acc_ref[:, side * half : (side + 1) * half] += lax.dot_general(
            h, ref[...].reshape(half, hid), (((1,), (1,)), ((), ())), preferred_element_type=jnp.float32
        )

    @pl.when(e == pl.num_programs(0) - 1)
    def _():
        out_ref[...] = acc_ref[...].astype(out_ref.dtype)


def down_product(info, hidden, down):
    experts, blocks, rows, hid = down[0].shape
    tokens = hidden.shape[0]
    width = 2 * blocks * rows
    weight = pl.BlockSpec((1, blocks, rows, hid), lambda e: (e, 0, 0, 0))
    return pl.pallas_call(
        down_kernel,
        grid=(experts,),
        in_specs=[
            pl.BlockSpec(info.shape, lambda e: (0, 0)),
            pl.BlockSpec(hidden.shape, lambda e: (0, 0)),
            weight,
            weight,
        ],
        out_specs=pl.BlockSpec((tokens, width), lambda e: (0, 0)),
        out_shape=jax.ShapeDtypeStruct((tokens, width), jnp.bfloat16),
        scratch_shapes=[pltpu.VMEM((tokens, width), jnp.float32)],
        cost_estimate=pl.CostEstimate(
            flops=experts * 2 * tokens * width * hid, transcendentals=0, bytes_accessed=2 * down[0].size * 2
        ),
        name="down",
    )(info, hidden, down[0], down[1])


def make_shards(groups, owners):
    cores = 2
    planes = owners // cores

    def flat(g, z, c):
        return (g * planes + z) * cores + c

    def route(move):
        pairs = []
        for g in range(groups):
            for z in range(planes):
                for c in range(cores):
                    to = move(g, z, c)
                    if to is not None:
                        pairs.append((flat(g, z, c), flat(*to)))
        return pairs

    def across(value, m):
        return lax.ppermute(value, AXES, route(lambda g, z, c: (g ^ m, z, c)))

    def along(value, m):
        return lax.ppermute(value, AXES, route(lambda g, z, c: (g, z ^ m, c)))

    def swap(value):
        return lax.ppermute(value, AXES, route(lambda g, z, c: (g, z, c ^ 1)))

    def upward(value, senders):
        return lax.ppermute(value, AXES, route(lambda g, z, c: (g, z + 1, c) if z in senders else None))

    def downward(value, senders):
        return lax.ppermute(value, AXES, route(lambda g, z, c: (g, z - 1, c) if z in senders else None))

    def shards(tokens, routes, router_weight, shift, scale, gate_mod, gate_weight, up_weight, down_weight):
        tok_dev, width = tokens.shape
        experts, rows, hidden_all = gate_weight.shape
        hid = hidden_all // groups
        g = lax.axis_index("dp")
        owner = lax.axis_index("expert")
        z, c = owner // cores, owner % cores
        quarter = width // planes

        def pick(slots, choice):
            names = sorted(set(choice.values()))
            value = slots[names[0]]
            for name in names[1:]:
                here = jnp.zeros((), jnp.bool_)
                for plane, slot in choice.items():
                    if slot == name:
                        here = here | (z == plane)
                value = jnp.where(here, slots[name], value)
            return value

        def share(weight):
            def part(m):
                return lax.dynamic_slice_in_dim(weight, (g ^ m) * hid, hid, 2)

            return [part(0)] + [across(part(m), m) for m in range(1, groups)]

        def gather(parts):
            full = jnp.zeros((experts, groups, rows, hid), jnp.bfloat16)
            for m, part in enumerate(parts):
                full = lax.dynamic_update_slice(full, part[:, None], (0, g ^ m, 0, 0))
            return full, swap(full)

        gate_parts = share(gate_weight)
        up_parts = share(up_weight)

        first_row = flat(g, z, c) * tok_dev
        image = first_row // PIX
        shift_row = lax.dynamic_slice_in_dim(shift, image, 1, 0)
        scale_row = lax.dynamic_slice_in_dim(scale, image, 1, 0)
        values = tokens.astype(jnp.float32)
        meansq = jnp.mean(values * values, axis=-1, keepdims=True)
        normed = (values * lax.rsqrt(meansq + EPS) * (1.0 + scale_row) + shift_row).astype(jnp.bfloat16)

        fine = normed.reshape(tok_dev, groups, planes, cores, rows)

        def features(plane):
            own = lax.dynamic_slice(fine, (0, 0, plane, c, 0), (tok_dev, groups, 1, 1, rows))
            other = lax.dynamic_slice(fine, (0, 0, plane, 1 - c, 0), (tok_dev, groups, 1, 1, rows))
            return jnp.concatenate([own.reshape(tok_dev, -1), other.reshape(tok_dev, -1)], axis=1)

        sent = {m: along(features(z ^ m), m) for m in range(planes - 1, 0, -1)}
        sent[0] = features(z)

        logits = jnp.dot(normed, router_weight, preferred_element_type=jnp.float32)
        onehot = routes[:, :, None] == jnp.arange(experts, dtype=jnp.int32)[None, None, :]
        score = jax.nn.sigmoid(jnp.sum(jnp.where(onehot, logits[:, None, :], 0.0), axis=-1))
        info = jnp.concatenate([routes.astype(jnp.float32), score], axis=1).T
        every = lax.all_gather(info, AXES, axis=0, tiled=False)

        def info_of(m):
            who = jnp.stack([flat(g ^ b, z ^ m, c) for b in range(groups)])
            return every[who].transpose(0, 2, 1).reshape(groups * tok_dev, 4)

        infos = {m: info_of(m) for m in range(planes)}
        gate_full = gather(gate_parts)
        up_full = gather(up_parts)

        partial = {}
        for m in range(planes - 1, -1, -1):
            block = jnp.concatenate([sent[m]] + [across(sent[m], b) for b in range(1, groups)], axis=0)
            partial[m] = gate_up(infos[m], block, gate_full, up_full)

        from_below = from_above = None
        for s in range(1, planes):
            climb = {p: p ^ (planes - s + p) for p in range(0, s)}
            sink = {p: p ^ (s - planes + p) for p in range(planes - s, planes)}
            rising, falling = pick(partial, climb), pick(partial, sink)
            if from_below is not None:
                rising = (rising.astype(jnp.float32) + from_below.astype(jnp.float32)).astype(jnp.bfloat16)
                falling = (falling.astype(jnp.float32) + from_above.astype(jnp.float32)).astype(jnp.bfloat16)
            from_below, from_above = upward(rising, set(climb)), downward(falling, set(sink))
        total = partial[0].astype(jnp.float32)
        if planes > 1:
            total = total + from_below.astype(jnp.float32) + from_above.astype(jnp.float32)
        hidden = jnp.concatenate(
            [
                jax.nn.silu(total[:, 2 * k * hid : (2 * k + 1) * hid])
                * total[:, (2 * k + 1) * hid : (2 * k + 2) * hid]
                * infos[0][:, 2 + k : 3 + k]
                for k in range(2)
            ],
            axis=1,
        ).astype(jnp.bfloat16)

        down_full = gather(share(down_weight))

        below, above = [hidden], [hidden]
        for s in range(1, planes):
            below.append(upward(below[-1], set(range(s - 1, planes - 1))))
            above.append(downward(above[-1], set(range(1, planes - s + 1))))

        gate_fine = lax.dynamic_slice_in_dim(gate_mod, 0, gate_mod.shape[0], 0).reshape(
            gate_mod.shape[0], groups, planes, cores, rows
        )

        def gate_row(m):
            its_image = flat(g, z ^ m, c) * tok_dev // PIX
            own = lax.dynamic_slice(gate_fine, (its_image, 0, z, c, 0), (1, groups, 1, 1, rows))
            other = lax.dynamic_slice(gate_fine, (its_image, 0, z, 1 - c, 0), (1, groups, 1, 1, rows))
            return jnp.concatenate([own.reshape(1, -1), other.reshape(1, -1)], axis=1)

        finished = {}
        for m in range(planes):
            lower = {p: p - (p ^ m) for p in range(planes) if (p ^ m) < p}
            upper_ = {p: (p ^ m) - p for p in range(planes) if (p ^ m) > p}
            if m == 0:
                rows_in = hidden
            else:
                rows_in = jnp.where(z > (z ^ m), pick(below, lower), pick(above, upper_))
            out = down_product(infos[m], rows_in, down_full).reshape(groups, tok_dev, quarter)
            gathered = out[0].astype(jnp.float32)
            for b in range(1, groups):
                gathered = gathered + across(out[b], b).astype(jnp.float32)
            piece = (gathered * gate_row(m)).astype(jnp.bfloat16)
            finished[m] = along(piece, m) if m else piece

        update = jnp.zeros((tok_dev, groups, planes, cores, rows), jnp.bfloat16)
        for m in range(planes):
            for side in range(2):
                piece = finished[m][:, side * (quarter // 2) : (side + 1) * (quarter // 2)]
                piece = piece.reshape(tok_dev, groups, 1, 1, rows)
                place = c if side == 0 else 1 - c
                update = lax.dynamic_update_slice(update, piece, (0, 0, z ^ m, place, 0))
        return update.reshape(tok_dev, width)

    return shards


def solution(mesh):
    rows = P(AXES, None)
    weights = P(None, AXES, None)
    in_specs = (rows, rows, P(), P(), P(), P(), weights, weights, weights)
    shards = make_shards(mesh.shape["dp"], mesh.shape["expert"])
    return jax.shard_map(shards, mesh=mesh, in_specs=in_specs, out_specs=rows, check_vma=False)
```

```python
import jax
import jax.numpy as jnp
from jax import lax
from jax.experimental import pallas as pl
from jax.experimental.pallas import tpu as pltpu
from jax.sharding import PartitionSpec as P

PIX = 4096
EPS = 1e-06
AXES = ("dp", "expert")
CORES = 2
LANES = 128


def send_back(output):
    return lax.all_to_all(output, "expert", split_axis=0, concat_axis=0, tiled=True)


def routed_shards(
    tokens, routes, router_weight, shift, scale, gate_mod, gate_weight, up_weight, down_weight
):
    tok_dev = tokens.shape[0]
    width = tokens.shape[1]
    experts = router_weight.shape[1]
    n_owner = lax.axis_size("expert")
    local_count = experts // n_owner
    capacity = max(2, 3 * tok_dev // experts)
    first_row = (lax.axis_index("dp") * n_owner + lax.axis_index("expert")) * tok_dev
    image = first_row // PIX
    shift_row = lax.dynamic_slice_in_dim(shift, image, 1, 0)
    scale_row = lax.dynamic_slice_in_dim(scale, image, 1, 0)
    gate_row = lax.dynamic_slice_in_dim(gate_mod, image, 1, 0)
    values = tokens.astype(jnp.float32)
    meansq = jnp.mean(values * values, axis=-1, keepdims=True)
    normed = (values * lax.rsqrt(meansq + EPS) * (1.0 + scale_row) + shift_row).astype(jnp.bfloat16)
    logits = jnp.dot(normed, router_weight, preferred_element_type=jnp.float32)
    onehot = routes[:, :, None] == jnp.arange(experts, dtype=jnp.int32)[None, None, :]
    chosen = jnp.sum(jnp.where(onehot, logits[:, None, :], 0.0), axis=-1)
    score = jax.nn.sigmoid(chosen)
    flat = routes.reshape(-1)
    hot = (flat[:, None] == jnp.arange(experts, dtype=jnp.int32)[None, :]).astype(jnp.int32)
    rank = jnp.cumsum(hot, axis=0) - hot
    slot = jnp.sum(rank * hot, axis=-1)
    position = flat * capacity + slot
    source = (
        jnp.zeros((experts * capacity,), jnp.int32)
        .at[position]
        .set(jnp.arange(2 * tok_dev, dtype=jnp.int32) // 2)
    )
    filled = jnp.zeros((experts * capacity,), jnp.bool_).at[position].set(True)
    outgoing = jnp.where(filled[:, None], normed[source], jnp.zeros((), jnp.bfloat16)).reshape(
        experts, capacity, width
    )
    quarter_gate, quarter_up, quarter_down = (
        lax.all_to_all(gate_weight, "expert", split_axis=0, concat_axis=1, tiled=True),
        lax.all_to_all(up_weight, "expert", split_axis=0, concat_axis=1, tiled=True),
        lax.all_to_all(down_weight, "expert", split_axis=0, concat_axis=1, tiled=True),
    )
    w_gate, w_up, w_down = (
        lax.all_gather(quarter_gate, "dp", axis=1, tiled=True),
        lax.all_gather(quarter_up, "dp", axis=1, tiled=True),
        lax.all_gather(quarter_down, "dp", axis=1, tiled=True),
    )
    received = lax.all_to_all(outgoing, "expert", split_axis=0, concat_axis=0, tiled=True)
    slots = received.shape[1]
    grid = received.reshape(n_owner, local_count, slots, width)
    gate = jnp.einsum("nxcd,xdf->nxcf", grid, w_gate, preferred_element_type=jnp.float32)
    upper = jnp.einsum("nxcd,xdf->nxcf", grid, w_up, preferred_element_type=jnp.float32)
    hidden = (jax.nn.silu(gate) * upper).astype(jnp.bfloat16)
    output = jnp.einsum(
        "nxcf,xdf->nxcd", hidden, w_down, preferred_element_type=jnp.float32
    ).astype(jnp.bfloat16)
    output = output.reshape(n_owner * local_count, slots, width)
    incoming = send_back(output)
    picked = (
        incoming.reshape(experts * capacity, width)[position]
        .astype(jnp.float32)
        .reshape(tok_dev, 2, width)
    )
    branch = jnp.sum(score[:, :, None] * picked, axis=1)
    return (gate_row * branch).astype(jnp.bfloat16)


def prep_kernel(here, tok_ref, routes_ref, router_ref, shift_ref, scale_ref, *refs):
    outs, norm_ref = refs[:-1], refs[-1]
    z, c = here[1], here[2]
    planes = len(outs)
    tokens, width = tok_ref.shape
    quarter = width // planes
    experts = router_ref.shape[0]
    values = tok_ref[...].astype(jnp.float32)
    meansq = jnp.mean(values * values, axis=-1, keepdims=True)
    normed = values * lax.rsqrt(meansq + EPS) * (1.0 + scale_ref[...]) + shift_ref[...]
    normed = normed.astype(jnp.bfloat16)
    norm_ref[...] = normed
    logits = lax.dot_general(
        normed, router_ref[...], (((1,), (1,)), ((), ())), preferred_element_type=jnp.float32
    )
    ids = lax.broadcasted_iota(jnp.int32, (tokens, experts), 1)
    lane = lax.broadcasted_iota(jnp.int32, (tokens, LANES), 1)
    info = jnp.zeros((tokens, LANES), jnp.float32)
    for k in range(2):
        expert = routes_ref[:, k : k + 1]
        chosen = jnp.sum(jnp.where(ids == expert, logits, 0.0), axis=-1, keepdims=True)
        score = jax.nn.sigmoid(chosen)
        coarse = score.astype(jnp.bfloat16).astype(jnp.float32)
        info = jnp.where(lane == k, expert.astype(jnp.float32), info)
        info = jnp.where(lane == 2 + 2 * k, coarse, info)
        info = jnp.where(lane == 3 + 2 * k, score - coarse, info)
    info = info.astype(jnp.bfloat16)
    rows = LANES
    groups = quarter // (CORES * rows)
    for m, out in enumerate(outs):
        for side in range(CORES):
            for b in range(groups):
                start = ((b * planes + (z ^ m)) * CORES + (c ^ side)) * rows
                at = (side * groups + b) * rows
                out[:, at : at + rows] = norm_ref[:, pl.ds(pl.multiple_of(start, LANES), rows)]
        out[:, quarter:] = info


def prep(here, tokens, routes, router, shift_row, scale_row, planes):
    rows, width = tokens.shape
    block = jax.ShapeDtypeStruct((rows, width // planes + LANES), jnp.bfloat16)
    vmem = pl.BlockSpec(memory_space=pltpu.VMEM)
    return pl.pallas_call(
        prep_kernel,
        in_specs=[pl.BlockSpec(memory_space=pltpu.SMEM)] + [vmem] * 5,
        out_specs=[vmem] * planes,
        out_shape=[block] * planes,
        scratch_shapes=[pltpu.VMEM((rows, width), jnp.bfloat16)],
        name="prep",
    )(here, tokens, routes, router, shift_row, scale_row)


def gate_up_kernel(groups, here, *refs):
    blocks, (gate_a, gate_b, up_a, up_b, out_ref, x_ref, route_ref) = refs[:groups], refs[groups:]
    e = pl.program_id(0)
    hid = gate_a.shape[-1]
    tile = blocks[0].shape[0]
    depth = x_ref.shape[1]
    half = depth // CORES

    @pl.when(e == 0)
    def _():
        for i, block in enumerate(blocks):
            at = slice(i * tile, (i + 1) * tile)
            for side in range(CORES):
                for m in range(groups):
                    start = pl.multiple_of((side * groups + (here[0] ^ m)) * LANES, LANES)
                    to = (side * groups + m) * LANES
                    x_ref[at, to : to + LANES] = block[:, pl.ds(start, LANES)]
            for k in range(2):
                route = block[:, depth + k : depth + k + 1].astype(jnp.float32)
                route_ref[at, k * hid : (k + 1) * hid] = jnp.broadcast_to(route, (tile, hid)).astype(jnp.bfloat16)

    mine = e.astype(jnp.float32).astype(jnp.bfloat16)
    gate_w = jnp.concatenate([gate_a[...].reshape(half, hid), gate_b[...].reshape(half, hid)], axis=0)
    up_w = jnp.concatenate([up_a[...].reshape(half, hid), up_b[...].reshape(half, hid)], axis=0)
    step = 2 * tile
    for start in range(0, x_ref.shape[0], step):
        at = slice(start, start + step)
        for part, weight in enumerate((gate_w, up_w)):
            product = jnp.dot(x_ref[at, :], weight, preferred_element_type=jnp.float32).astype(jnp.bfloat16)
            for k in range(2):
                to = slice((2 * k + part) * hid, (2 * k + part + 1) * hid)
                chosen = route_ref[at, k * hid : (k + 1) * hid] == mine
                out_ref[at, to] = jnp.where(chosen, product, out_ref[at, to])


def gate_up(here, blocks, gate, up):
    groups, experts, rows, hid = gate[0].shape
    tile, lanes = blocks[0].shape
    tokens = groups * tile
    depth = lanes - LANES
    weight = pl.BlockSpec((groups, 1, rows, hid), lambda e: (0, e, 0, 0))
    return pl.pallas_call(
        lambda *refs: gate_up_kernel(groups, *refs),
        grid=(experts,),
        in_specs=[pl.BlockSpec(memory_space=pltpu.SMEM)]
        + [pl.BlockSpec((tile, lanes), lambda e: (0, 0))] * groups
        + [weight] * 4,
        out_specs=pl.BlockSpec((tokens, 4 * hid), lambda e: (0, 0)),
        out_shape=jax.ShapeDtypeStruct((tokens, 4 * hid), jnp.bfloat16),
        scratch_shapes=[
            pltpu.VMEM((tokens, depth), jnp.bfloat16),
            pltpu.VMEM((tokens, 2 * hid), jnp.bfloat16),
        ],
        cost_estimate=pl.CostEstimate(
            flops=experts * 4 * tokens * depth * hid, transcendentals=0, bytes_accessed=4 * gate[0].size * 2
        ),
        name="gate_up",
    )(here, *blocks, gate[0], gate[1], up[0], up[1])


def hidden_kernel(groups, count, *refs):
    parts, infos, out_ref = refs[:count], refs[count : count + groups], refs[-1]
    hid = out_ref.shape[1] // 2
    tile = infos[0].shape[0]
    for i, info in enumerate(infos):
        at = slice(i * tile, (i + 1) * tile)
        for k in range(2):
            score = info[:, 2 + 2 * k : 3 + 2 * k].astype(jnp.float32) + info[:, 3 + 2 * k : 4 + 2 * k].astype(jnp.float32)
            sums = []
            for part in range(2):
                to = slice((2 * k + part) * hid, (2 * k + part + 1) * hid)
                total = parts[0][at, to].astype(jnp.float32)
                for other in parts[1:]:
                    total = total + other[at, to].astype(jnp.float32)
                sums.append(total)
            value = sums[0] / (1.0 + jnp.exp(-sums[0])) * sums[1] * score
            out_ref[at, k * hid : (k + 1) * hid] = value.astype(jnp.bfloat16)


def hidden_rows(parts, blocks, hid):
    groups = len(blocks)
    tile, lanes = blocks[0].shape
    tokens = groups * tile
    last = lanes // LANES - 1
    return pl.pallas_call(
        lambda *refs: hidden_kernel(groups, len(parts), *refs),
        grid=(1,),
        in_specs=[pl.BlockSpec((tokens, 4 * hid), lambda i: (0, 0))] * len(parts)
        + [pl.BlockSpec((tile, LANES), lambda i: (0, last))] * groups,
        out_specs=pl.BlockSpec((tokens, 2 * hid), lambda i: (0, 0)),
        out_shape=jax.ShapeDtypeStruct((tokens, 2 * hid), jnp.bfloat16),
        name="hidden",
    )(*parts, *blocks)


def down_kernel(groups, experts, here, h_ref, *refs):
    infos, refs = refs[:groups], refs[groups:]
    down_a, down_b, outs, wide_ref = refs[0], refs[1], refs[2 : 2 + groups], refs[-1]
    j = pl.program_id(0)
    hid = h_ref.shape[1] // 2
    tile = infos[0].shape[0]
    pair = down_a.shape[0]
    zero = jnp.zeros((), jnp.bfloat16)

    @pl.when(j == 0)
    def _():
        for i, info in enumerate(infos):
            at = slice(i * tile, (i + 1) * tile)
            routes = [jnp.broadcast_to(info[:, k : k + 1], (tile, hid)) for k in range(2)]
            for e in range(experts):
                mine = jnp.array(e, jnp.bfloat16)
                value = jnp.where(routes[0] == mine, h_ref[at, :hid], zero)
                value = jnp.where(routes[1] == mine, h_ref[at, hid:], value)
                wide_ref[at, e * hid : (e + 1) * hid] = value

    for side, ref in enumerate((down_a, down_b)):
        weight = jnp.concatenate(
            [jnp.concatenate([ref[p, e] for p in range(pair)], axis=0) for e in range(experts)], axis=1
        )
        product = lax.dot_general(
            wide_ref[...], weight, (((1,), (1,)), ((), ())), preferred_element_type=jnp.float32
        ).astype(jnp.bfloat16)
        for p in range(pair):
            start = pl.multiple_of((side * groups + (here[0] ^ (j * pair + p))) * LANES, LANES)
            for i, out in enumerate(outs):
                out[:, pl.ds(start, LANES)] = product[i * tile : (i + 1) * tile, p * LANES : (p + 1) * LANES]


def down_product(here, hidden, blocks, down):
    groups, experts, rows, hid = down[0].shape
    tile, lanes = blocks[0].shape
    tokens = groups * tile
    last = lanes // LANES - 1
    width = lanes - LANES
    pair = 2 if groups % 2 == 0 else 1
    weight = pl.BlockSpec((pair, experts, rows, hid), lambda j: (j, 0, 0, 0))
    return pl.pallas_call(
        lambda *refs: down_kernel(groups, experts, *refs),
        grid=(groups // pair,),
        in_specs=[pl.BlockSpec(memory_space=pltpu.SMEM), pl.BlockSpec(hidden.shape, lambda j: (0, 0))]
        + [pl.BlockSpec((tile, LANES), lambda j: (0, last))] * groups
        + [weight] * 2,
        out_specs=[pl.BlockSpec((tile, width), lambda j: (0, 0))] * groups,
        out_shape=[jax.ShapeDtypeStruct((tile, width), jnp.bfloat16)] * groups,
        scratch_shapes=[pltpu.VMEM((tokens, experts * hid), jnp.bfloat16)],
        cost_estimate=pl.CostEstimate(
            flops=experts * 2 * tokens * width * hid, transcendentals=0, bytes_accessed=2 * down[0].size * 2
        ),
        name="down",
    )(here, hidden, *blocks, *down)


def combine_kernel(groups, planes, here, gate_ref, *refs):
    parts, out_ref = refs[:-1], refs[-1]
    z, c = here[1], here[2]
    for side in range(CORES):
        for b in range(groups):
            to = slice((side * groups + b) * LANES, (side * groups + b + 1) * LANES)
            total = parts[0][:, to].astype(jnp.float32)
            for part in parts[1:]:
                total = total + part[:, to].astype(jnp.float32)
            start = pl.multiple_of(((b * planes + z) * CORES + (c ^ side)) * LANES, LANES)
            out_ref[:, to] = (total * gate_ref[:, pl.ds(start, LANES)]).astype(jnp.bfloat16)


def combine(here, gate_row, parts, planes):
    vmem = pl.BlockSpec(memory_space=pltpu.VMEM)
    return pl.pallas_call(
        lambda *refs: combine_kernel(len(parts), planes, *refs),
        in_specs=[pl.BlockSpec(memory_space=pltpu.SMEM)] + [vmem] * (1 + len(parts)),
        out_specs=vmem,
        out_shape=jax.ShapeDtypeStruct(parts[0].shape, jnp.bfloat16),
        name="combine",
    )(here, gate_row, *parts)


def place_kernel(groups, here, *refs):
    pieces, out_ref = refs[:-1], refs[-1]
    planes = len(pieces)
    z, c = here[1], here[2]
    for m, piece in enumerate(pieces):
        for side in range(CORES):
            for b in range(groups):
                start = pl.multiple_of(((b * planes + (z ^ m)) * CORES + (c ^ side)) * LANES, LANES)
                at = (side * groups + b) * LANES
                out_ref[:, pl.ds(start, LANES)] = piece[:, at : at + LANES]


def place(here, pieces, groups):
    tokens, quarter = pieces[0].shape
    vmem = pl.BlockSpec(memory_space=pltpu.VMEM)
    return pl.pallas_call(
        lambda *refs: place_kernel(groups, *refs),
        in_specs=[pl.BlockSpec(memory_space=pltpu.SMEM)] + [vmem] * len(pieces),
        out_specs=vmem,
        out_shape=jax.ShapeDtypeStruct((tokens, quarter * len(pieces)), jnp.bfloat16),
        name="place",
    )(here, *pieces)


def plane_shards(groups, owners):
    planes = owners // CORES

    def flat(g, z, c):
        return (g * planes + z) * CORES + c

    def permute(value, move):
        pairs = []
        for g in range(groups):
            for z in range(planes):
                for c in range(CORES):
                    to = move(g, z, c)
                    if to is not None:
                        pairs.append((flat(g, z, c), flat(*to)))
        return lax.ppermute(value, AXES, pairs)

    def across(value, m):
        return permute(value, lambda g, z, c: (g ^ m, z, c))

    def along(value, m):
        return permute(value, lambda g, z, c: (g, z ^ m, c))

    def swap(value):
        return permute(value, lambda g, z, c: (g, z, c ^ 1))

    def upward(value, senders):
        return permute(value, lambda g, z, c: (g, z + 1, c) if z in senders else None)

    def downward(value, senders):
        return permute(value, lambda g, z, c: (g, z - 1, c) if z in senders else None)

    def add(first, second):
        return (first.astype(jnp.float32) + second.astype(jnp.float32)).astype(jnp.bfloat16)

    def shards(tokens, routes, router_weight, shift, scale, gate_mod, gate_weight, up_weight, down_weight):
        tok_dev = tokens.shape[0]
        hid = gate_weight.shape[2] // groups
        g = lax.axis_index("dp")
        owner = lax.axis_index("expert")
        z, c = owner // CORES, owner % CORES
        here = jnp.stack([g, z, c]).astype(jnp.int32)

        def among(names):
            found = jnp.zeros((), jnp.bool_)
            for plane in names:
                found = found | (z == plane)
            return found

        def pick(slots, choice):
            names = sorted(set(choice.values()))
            value = slots[names[0]]
            for name in names[1:]:
                value = jnp.where(among([p for p, slot in choice.items() if slot == name]), slots[name], value)
            return value

        def row_of(table, m):
            image = flat(g, z ^ m, c) * tok_dev // PIX
            return lax.dynamic_slice_in_dim(table, image, 1, 0)

        def share(weight):
            def part(m):
                return lax.dynamic_slice_in_dim(weight, (g ^ m) * hid, hid, 2)

            return [part(0)] + [across(part(m), m) for m in range(1, groups)]

        def gather(parts):
            full = jnp.stack(parts)
            return full, swap(full)

        gate_parts = share(gate_weight)
        up_parts = share(up_weight)
        split = prep(here, tokens, routes, router_weight.T, row_of(shift, 0), row_of(scale, 0), planes)
        sent = {m: along(split[m], m) for m in range(planes - 1, 0, -1)}
        sent[0] = split[0]
        gate_full = gather(gate_parts)
        up_full = gather(up_parts)

        partial, blocks = {}, {}
        for m in range(planes - 1, -1, -1):
            blocks[m] = [sent[m]] + [across(sent[m], b) for b in range(1, groups)]
            partial[m] = gate_up(here, blocks[m], gate_full, up_full)

        below = above = None
        for s in range(1, planes):
            climb = {p: p ^ (planes - s + p) for p in range(0, s)}
            sink = {p: p ^ (s - planes + p) for p in range(planes - s, planes)}
            if set(climb) & set(sink):
                rising, falling = pick(partial, climb), pick(partial, sink)
                if below is not None:
                    rising, falling = add(rising, below), add(falling, above)
            else:
                rising = pick(partial, {**climb, **sink})
                if below is not None:
                    rising = add(rising, jnp.where(among(climb), below, above))
                falling = rising
            below, above = upward(rising, set(climb)), downward(falling, set(sink))
        hidden = hidden_rows([partial[0]] + ([below, above] if planes > 1 else []), blocks[0], hid)

        down_full = gather(share(down_weight))

        from_below, from_above = [hidden], [hidden]
        for s in range(1, planes):
            from_below.append(upward(from_below[-1], set(range(s - 1, planes - 1))))
            from_above.append(downward(from_above[-1], set(range(1, planes - s + 1))))

        finished = []
        for m in range(planes):
            rows_in = hidden
            if m:
                lower = {p: p - (p ^ m) for p in range(planes) if (p ^ m) < p}
                upper = {p: (p ^ m) - p for p in range(planes) if (p ^ m) > p}
                rows_in = jnp.where(among(lower), pick(from_below, lower), pick(from_above, upper))
            out = down_product(here, rows_in, blocks[m], down_full)
            piece = combine(here, row_of(gate_mod, m), [out[0]] + [across(out[b], b) for b in range(1, groups)], planes)
            finished.append(along(piece, m) if m else piece)
        return place(here, finished, groups)

    return shards


def solution(mesh):
    groups, owners = mesh.shape["dp"], mesh.shape["expert"]

    def program(tokens, routes, router_weight, shift, scale, gate_mod, gate_weight, up_weight, down_weight):
        rows = P(AXES, None)
        weights = P(None, AXES, None)
        in_specs = (rows, rows, P(), P(), P(), P(), weights, weights, weights)
        planes = owners // CORES
        whole_lanes = gate_weight.shape[1] == LANES * groups * owners
        powers = groups & (groups - 1) == 0 and planes & (planes - 1) == 0 and owners == planes * CORES
        body = plane_shards(groups, owners) if whole_lanes and powers else routed_shards
        step = jax.shard_map(body, mesh=mesh, in_specs=in_specs, out_specs=rows, check_vma=False)
        return step(tokens, routes, router_weight, shift, scale, gate_mod, gate_weight, up_weight, down_weight)

    return program
```

```python
import jax
import jax.numpy as jnp
from jax import lax
from jax.experimental import pallas as pl
from jax.experimental.pallas import tpu as pltpu
from jax.sharding import PartitionSpec as P


PIX = 4096
EPS = 1e-06
AXES = ("dp", "expert")
CORES = 2
LANES = 128


def send_back(output):
    return lax.all_to_all(output, "expert", split_axis=0, concat_axis=0, tiled=True)


def routed_shards(
    tokens, routes, router_weight, shift, scale, gate_mod, gate_weight, up_weight, down_weight
):
    tok_dev = tokens.shape[0]
    width = tokens.shape[1]
    experts = router_weight.shape[1]
    n_owner = lax.axis_size("expert")
    local_count = experts // n_owner
    capacity = max(2, 3 * tok_dev // experts)
    first_row = (lax.axis_index("dp") * n_owner + lax.axis_index("expert")) * tok_dev
    image = first_row // PIX
    shift_row = lax.dynamic_slice_in_dim(shift, image, 1, 0)
    scale_row = lax.dynamic_slice_in_dim(scale, image, 1, 0)
    gate_row = lax.dynamic_slice_in_dim(gate_mod, image, 1, 0)
    values = tokens.astype(jnp.float32)
    meansq = jnp.mean(values * values, axis=-1, keepdims=True)
    normed = (values * lax.rsqrt(meansq + EPS) * (1.0 + scale_row) + shift_row).astype(jnp.bfloat16)
    logits = jnp.dot(normed, router_weight, preferred_element_type=jnp.float32)
    onehot = routes[:, :, None] == jnp.arange(experts, dtype=jnp.int32)[None, None, :]
    chosen = jnp.sum(jnp.where(onehot, logits[:, None, :], 0.0), axis=-1)
    score = jax.nn.sigmoid(chosen)
    flat = routes.reshape(-1)
    hot = (flat[:, None] == jnp.arange(experts, dtype=jnp.int32)[None, :]).astype(jnp.int32)
    rank = jnp.cumsum(hot, axis=0) - hot
    slot = jnp.sum(rank * hot, axis=-1)
    position = flat * capacity + slot
    source = (
        jnp.zeros((experts * capacity,), jnp.int32)
        .at[position]
        .set(jnp.arange(2 * tok_dev, dtype=jnp.int32) // 2)
    )
    filled = jnp.zeros((experts * capacity,), jnp.bool_).at[position].set(True)
    outgoing = jnp.where(filled[:, None], normed[source], jnp.zeros((), jnp.bfloat16)).reshape(
        experts, capacity, width
    )
    quarter_gate, quarter_up, quarter_down = (
        lax.all_to_all(gate_weight, "expert", split_axis=0, concat_axis=1, tiled=True),
        lax.all_to_all(up_weight, "expert", split_axis=0, concat_axis=1, tiled=True),
        lax.all_to_all(down_weight, "expert", split_axis=0, concat_axis=1, tiled=True),
    )
    w_gate, w_up, w_down = (
        lax.all_gather(quarter_gate, "dp", axis=1, tiled=True),
        lax.all_gather(quarter_up, "dp", axis=1, tiled=True),
        lax.all_gather(quarter_down, "dp", axis=1, tiled=True),
    )
    received = lax.all_to_all(outgoing, "expert", split_axis=0, concat_axis=0, tiled=True)
    slots = received.shape[1]
    grid = received.reshape(n_owner, local_count, slots, width)
    gate = jnp.einsum("nxcd,xdf->nxcf", grid, w_gate, preferred_element_type=jnp.float32)
    upper = jnp.einsum("nxcd,xdf->nxcf", grid, w_up, preferred_element_type=jnp.float32)
    hidden = (jax.nn.silu(gate) * upper).astype(jnp.bfloat16)
    output = jnp.einsum(
        "nxcf,xdf->nxcd", hidden, w_down, preferred_element_type=jnp.float32
    ).astype(jnp.bfloat16)
    output = output.reshape(n_owner * local_count, slots, width)
    incoming = send_back(output)
    picked = (
        incoming.reshape(experts * capacity, width)[position]
        .astype(jnp.float32)
        .reshape(tok_dev, 2, width)
    )
    branch = jnp.sum(score[:, :, None] * picked, axis=1)
    return (gate_row * branch).astype(jnp.bfloat16)


def prep_kernel(here, tok_ref, routes_ref, router_ref, shift_ref, scale_ref, *refs):
    outs, norm_ref = refs[:-1], refs[-1]
    z, c = here[1], here[2]
    planes = len(outs)
    tokens, width = tok_ref.shape
    quarter = width // planes
    experts = router_ref.shape[0]
    values = tok_ref[...].astype(jnp.float32)
    meansq = jnp.mean(values * values, axis=-1, keepdims=True)
    normed = values * lax.rsqrt(meansq + EPS) * (1.0 + scale_ref[...]) + shift_ref[...]
    normed = normed.astype(jnp.bfloat16)
    norm_ref[...] = normed
    logits = lax.dot_general(
        normed, router_ref[...], (((1,), (1,)), ((), ())), preferred_element_type=jnp.float32
    )
    ids = lax.broadcasted_iota(jnp.int32, (tokens, experts), 1)
    lane = lax.broadcasted_iota(jnp.int32, (tokens, LANES), 1)
    info = jnp.zeros((tokens, LANES), jnp.float32)
    for k in range(2):
        expert = routes_ref[:, k : k + 1]
        chosen = jnp.sum(jnp.where(ids == expert, logits, 0.0), axis=-1, keepdims=True)
        score = jax.nn.sigmoid(chosen)
        coarse = score.astype(jnp.bfloat16).astype(jnp.float32)
        info = jnp.where(lane == k, expert.astype(jnp.float32), info)
        info = jnp.where(lane == 2 + 2 * k, coarse, info)
        info = jnp.where(lane == 3 + 2 * k, score - coarse, info)
    info = info.astype(jnp.bfloat16)
    rows = LANES
    groups = quarter // (CORES * rows)
    for m, out in enumerate(outs):
        for side in range(CORES):
            for b in range(groups):
                start = ((b * planes + (z ^ m)) * CORES + (c ^ side)) * rows
                at = (side * groups + b) * rows
                out[:, at : at + rows] = norm_ref[:, pl.ds(pl.multiple_of(start, LANES), rows)]
        out[:, quarter:] = info


def prep(here, tokens, routes, router, shift_row, scale_row, planes):
    rows, width = tokens.shape
    block = jax.ShapeDtypeStruct((rows, width // planes + LANES), jnp.bfloat16)
    vmem = pl.BlockSpec(memory_space=pltpu.VMEM)
    return pl.pallas_call(
        prep_kernel,
        in_specs=[pl.BlockSpec(memory_space=pltpu.SMEM)] + [vmem] * 5,
        out_specs=[vmem] * planes,
        out_shape=[block] * planes,
        scratch_shapes=[pltpu.VMEM((rows, width), jnp.bfloat16)],
        name="prep",
    )(here, tokens, routes, router, shift_row, scale_row)


def product_kernel(groups, here, *refs):
    blocks, (first, second, out_ref, x_ref) = refs[:groups], refs[groups:]
    experts, hid = first.shape[1], first.shape[-1]
    tile = blocks[0].shape[0]
    depth = x_ref.shape[1]
    half = depth // CORES
    for i, block in enumerate(blocks):
        at = slice(i * tile, (i + 1) * tile)
        for side in range(CORES):
            for m in range(groups):
                start = pl.multiple_of((side * groups + (here[0] ^ m)) * LANES, LANES)
                to = (side * groups + m) * LANES
                x_ref[at, to : to + LANES] = block[:, pl.ds(start, LANES)]
    routes = [[block[:, depth + k : depth + k + 1].astype(jnp.float32) for k in range(2)] for block in blocks]
    for e in range(experts):
        weight = jnp.concatenate([first[:, e].reshape(half, hid), second[:, e].reshape(half, hid)], axis=0)
        product = jnp.dot(x_ref[...], weight, preferred_element_type=jnp.float32)
        for i in range(groups):
            at = slice(i * tile, (i + 1) * tile)
            for k in range(2):
                to = slice(k * hid, (k + 1) * hid)
                kept = out_ref[at, to].astype(jnp.float32)
                out_ref[at, to] = jnp.where(routes[i][k] == float(e), product[at], kept).astype(jnp.bfloat16)


def expert_product(here, blocks, weights):
    groups, experts, _, hid = weights[0].shape
    tile, lanes = blocks[0].shape
    tokens = groups * tile
    depth = lanes - LANES
    vmem = pl.BlockSpec(memory_space=pltpu.VMEM)
    return pl.pallas_call(
        lambda *refs: product_kernel(groups, *refs),
        in_specs=[pl.BlockSpec(memory_space=pltpu.SMEM)] + [vmem] * (groups + 2),
        out_specs=vmem,
        out_shape=jax.ShapeDtypeStruct((tokens, 2 * hid), jnp.bfloat16),
        scratch_shapes=[pltpu.VMEM((tokens, depth), jnp.bfloat16)],
        cost_estimate=pl.CostEstimate(
            flops=experts * 2 * tokens * depth * hid, transcendentals=0, bytes_accessed=4 * weights[0].size
        ),
        compiler_params=pltpu.CompilerParams(vmem_limit_bytes=24 * 2**20),
        name="product",
    )(here, *blocks, *weights)


def hidden_kernel(groups, count, *refs):
    parts, blocks, out_ref = refs[:count], refs[count : count + groups], refs[-1]
    hid = out_ref.shape[1] // 2
    tile, lanes = blocks[0].shape
    depth = lanes - LANES
    for i, block in enumerate(blocks):
        at = slice(i * tile, (i + 1) * tile)
        for k in range(2):
            score = [block[:, depth + 2 + 2 * k + n : depth + 3 + 2 * k + n].astype(jnp.float32) for n in range(2)]
            sums = []
            for part in range(2):
                to = slice((2 * k + part) * hid, (2 * k + part + 1) * hid)
                total = parts[0][at, to].astype(jnp.float32)
                for other in parts[1:]:
                    total = total + other[at, to].astype(jnp.float32)
                sums.append(total)
            value = sums[0] / (1.0 + jnp.exp(-sums[0])) * sums[1] * (score[0] + score[1])
            out_ref[at, k * hid : (k + 1) * hid] = value.astype(jnp.bfloat16)


def hidden_rows(parts, blocks):
    groups = len(blocks)
    tokens, columns = parts[0].shape
    vmem = pl.BlockSpec(memory_space=pltpu.VMEM)
    return pl.pallas_call(
        lambda *refs: hidden_kernel(groups, len(parts), *refs),
        in_specs=[vmem] * (len(parts) + groups),
        out_specs=vmem,
        out_shape=jax.ShapeDtypeStruct((tokens, columns // 2), jnp.bfloat16),
        cost_estimate=pl.CostEstimate(flops=10**9, transcendentals=0, bytes_accessed=4 * tokens * columns),
        name="hidden",
    )(*parts, *blocks)


def down_kernel(groups, experts, halves, here, *refs):
    hiddens, blocks, refs = refs[:halves], refs[halves : halves + groups], refs[halves + groups :]
    down_a, down_b, outs, wide_ref = refs[0], refs[1], refs[2 : 2 + groups], refs[-1]
    part = hiddens[0].shape[1] // 2
    hid = part * halves
    tile, lanes = blocks[0].shape
    depth = lanes - LANES
    pair = 2 if groups % 2 == 0 else 1
    zero = jnp.zeros((), jnp.float32)
    for i, block in enumerate(blocks):
        at = slice(i * tile, (i + 1) * tile)
        routes = [block[:, depth + k : depth + k + 1].astype(jnp.float32) for k in range(2)]
        for h, ref in enumerate(hiddens):
            rows = [ref[at, k * part : (k + 1) * part].astype(jnp.float32) for k in range(2)]
            for e in range(experts):
                value = jnp.where(routes[0] == float(e), rows[0], zero)
                value = jnp.where(routes[1] == float(e), rows[1], value)
                to = e * hid + h * part
                wide_ref[at, to : to + part] = value.astype(jnp.bfloat16)
    for side, ref in enumerate((down_a, down_b)):
        for j in range(0, groups, pair):
            weight = jnp.concatenate(
                [jnp.concatenate([ref[j + p, e] for p in range(pair)], axis=0) for e in range(experts)], axis=1
            )
            product = lax.dot_general(
                wide_ref[...], weight, (((1,), (1,)), ((), ())), preferred_element_type=jnp.float32
            ).astype(jnp.bfloat16)
            for p in range(pair):
                start = pl.multiple_of((side * groups + (here[0] ^ (j + p))) * LANES, LANES)
                for i, out in enumerate(outs):
                    out[:, pl.ds(start, LANES)] = product[i * tile : (i + 1) * tile, p * LANES : (p + 1) * LANES]


def down_product(here, hiddens, blocks, down):
    groups, experts, _, hid = down[0].shape
    tile, lanes = blocks[0].shape
    tokens = groups * tile
    width = lanes - LANES
    vmem = pl.BlockSpec(memory_space=pltpu.VMEM)
    return pl.pallas_call(
        lambda *refs: down_kernel(groups, experts, len(hiddens), *refs),
        in_specs=[pl.BlockSpec(memory_space=pltpu.SMEM)] + [vmem] * (len(hiddens) + groups + 2),
        out_specs=[vmem] * groups,
        out_shape=[jax.ShapeDtypeStruct((tile, width), jnp.bfloat16)] * groups,
        scratch_shapes=[pltpu.VMEM((tokens, experts * hid), jnp.bfloat16)],
        cost_estimate=pl.CostEstimate(
            flops=experts * 2 * tokens * width * hid, transcendentals=0, bytes_accessed=2 * down[0].size * 2
        ),
        compiler_params=pltpu.CompilerParams(vmem_limit_bytes=24 * 2**20),
        name="down",
    )(here, *hiddens, *blocks, *down)


def combine_kernel(groups, planes, here, gate_ref, *refs):
    parts, out_ref = refs[:-1], refs[-1]
    z, c = here[1], here[2]
    for side in range(CORES):
        for b in range(groups):
            to = slice((side * groups + b) * LANES, (side * groups + b + 1) * LANES)
            total = parts[0][:, to].astype(jnp.float32)
            for part in parts[1:]:
                total = total + part[:, to].astype(jnp.float32)
            start = pl.multiple_of(((b * planes + z) * CORES + (c ^ side)) * LANES, LANES)
            out_ref[:, to] = (total * gate_ref[:, pl.ds(start, LANES)]).astype(jnp.bfloat16)


def combine(here, gate_row, parts, planes):
    vmem = pl.BlockSpec(memory_space=pltpu.VMEM)
    return pl.pallas_call(
        lambda *refs: combine_kernel(len(parts), planes, *refs),
        in_specs=[pl.BlockSpec(memory_space=pltpu.SMEM)] + [vmem] * (1 + len(parts)),
        out_specs=vmem,
        out_shape=jax.ShapeDtypeStruct(parts[0].shape, jnp.bfloat16),
        name="combine",
    )(here, gate_row, *parts)


def place_kernel(groups, here, *refs):
    pieces, out_ref = refs[:-1], refs[-1]
    planes = len(pieces)
    z, c = here[1], here[2]
    for m, piece in enumerate(pieces):
        for side in range(CORES):
            for b in range(groups):
                start = pl.multiple_of(((b * planes + (z ^ m)) * CORES + (c ^ side)) * LANES, LANES)
                at = (side * groups + b) * LANES
                out_ref[:, pl.ds(start, LANES)] = piece[:, at : at + LANES]


def place(here, pieces, groups):
    tokens, quarter = pieces[0].shape
    vmem = pl.BlockSpec(memory_space=pltpu.VMEM)
    return pl.pallas_call(
        lambda *refs: place_kernel(groups, *refs),
        in_specs=[pl.BlockSpec(memory_space=pltpu.SMEM)] + [vmem] * len(pieces),
        out_specs=vmem,
        out_shape=jax.ShapeDtypeStruct((tokens, quarter * len(pieces)), jnp.bfloat16),
        name="place",
    )(here, *pieces)


def plane_shards(groups, owners):
    planes = owners // CORES

    def flat(g, z, c):
        return (g * planes + z) * CORES + c

    def permute(value, move):
        pairs = []
        for g in range(groups):
            for z in range(planes):
                for c in range(CORES):
                    to = move(g, z, c)
                    if to is not None:
                        pairs.append((flat(g, z, c), flat(*to)))
        return lax.ppermute(value, AXES, pairs)

    def across(value, m):
        return permute(value, lambda g, z, c: (g ^ m, z, c))

    def along(value, m):
        return permute(value, lambda g, z, c: (g, z ^ m, c))

    def swap(value):
        return permute(value, lambda g, z, c: (g, z, c ^ 1))

    def upward(value, senders):
        return permute(value, lambda g, z, c: (g, z + 1, c) if z in senders else None)

    def downward(value, senders):
        return permute(value, lambda g, z, c: (g, z - 1, c) if z in senders else None)

    def after(value, other):
        return lax.optimization_barrier((value, other))[0]

    def add(first, second):
        return (first.astype(jnp.float32) + second.astype(jnp.float32)).astype(jnp.bfloat16)

    def shards_of(tokens, routes, router_weight, shift, scale, gate_mod, gate_weight, up_weight, down_weight):
        tok_dev = tokens.shape[0]
        hid = gate_weight.shape[2] // groups
        g = lax.axis_index("dp")
        owner = lax.axis_index("expert")
        z, c = owner // CORES, owner % CORES
        here = jnp.stack([g, z, c]).astype(jnp.int32)

        def among(names):
            found = jnp.zeros((), jnp.bool_)
            for plane in names:
                found = found | (z == plane)
            return found

        def pick(slots, choice):
            names = sorted(set(choice.values()))
            value = slots[names[0]]
            for name in names[1:]:
                value = jnp.where(among([p for p, slot in choice.items() if slot == name]), slots[name], value)
            return value

        def row_of(table, m):
            image = flat(g, z ^ m, c) * tok_dev // PIX
            return lax.dynamic_slice_in_dim(table, image, 1, 0)

        def share(*weights, columns, start):
            def part(m):
                pieces = [lax.dynamic_slice_in_dim(w, (g ^ m) * hid + start, columns, 2) for w in weights]
                return jnp.concatenate(pieces, axis=2) if len(pieces) > 1 else pieces[0]

            return [part(0)] + [across(part(m), m) for m in range(1, groups)]

        far = planes - 1
        part = hid // 2
        order = list(range(far, -1, -1))

        parts0 = share(gate_weight, up_weight, columns=part, start=0)
        split = prep(here, tokens, routes, router_weight.T, row_of(shift, 0), row_of(scale, 0), planes)
        sent = {0: split[0]}
        for m in order[:-1]:
            sent[m] = along(split[m], m)
        parts1 = share(*after((gate_weight, up_weight), split), columns=part, start=part)
        blocks = {}
        for m in order:
            blocks[m] = [sent[m]] + [across(sent[m], b) for b in range(1, groups)]
        parts2 = share(after(down_weight, blocks[far]), columns=hid, start=0)

        def stack(parts, done):
            full = jnp.stack(after(parts, done) if done is not None else parts)
            return full, (full, swap(full))

        def multiply(m, weights, done):
            return expert_product(here, after(blocks[m], done), weights)

        def moved(s, partial, arrived, done):
            below, above = after(arrived, done) if arrived is not None else (None, None)
            climb = {p: p ^ (planes - s + p) for p in range(0, s)}
            sink = {p: p ^ (s - planes + p) for p in range(planes - s, planes)}
            if set(climb) & set(sink):
                rising, falling = pick(partial, climb), pick(partial, sink)
                if below is not None:
                    rising, falling = add(rising, below), add(falling, above)
            else:
                rising = pick(partial, {**climb, **sink})
                if below is not None:
                    rising = add(rising, jnp.where(among(climb), below, above))
                falling = rising
            return (upward(rising, set(climb)), downward(falling, set(sink))), (rising, falling)

        def activate(partial, arrived, done):
            return hidden_rows([partial[0], *after(arrived, done)], blocks[0])

        first, second = {}, {}
        last, weights0 = stack(parts0, None)
        first[far] = multiply(far, weights0, last)
        sum0, _ = moved(1, {m: first[far] for m in order}, None, None)
        last = first[far - 1] = multiply(far - 1, weights0, first[far])
        early = {m: first.get(m, last) for m in order}
        s = 2
        if planes > 3:
            sum0, last = moved(2, early, sum0, last)
            s = 3
        last, weights1 = stack(parts1, last)
        for m in order[2:-1]:
            last = first[m] = multiply(m, weights0, last)
        first[0] = first[far]
        for s in range(s, planes):
            sum0, last = moved(s, first, sum0, last)
        last = second[far] = multiply(far, weights1, last)
        sum1, _ = moved(1, {m: last for m in order}, None, None)
        last = second[far - 1] = multiply(far - 1, weights1, last)
        last = first[0] = multiply(0, weights0, last)
        hidden = {}
        last = hidden[0] = activate(first, sum0, last)
        early = {m: second.get(m, second[far]) for m in order}
        s = 2
        if planes > 3:
            sum1, last = moved(2, early, sum1, last)
            s = 3
        for m in order[2:-1]:
            last = second[m] = multiply(m, weights1, last)
        last, down_full = stack(parts2, last)
        last = second[0] = multiply(0, weights1, last)
        for s in range(s, planes):
            sum1, last = moved(s, second, sum1, last)
        last = hidden[1] = activate(second, sum1, last)

        rows_in = {(h, 0): hidden[h] for h in range(2)}
        for h in range(2):
            for m in order[:-1]:
                rows_in[h, m] = along(hidden[h], m)

        parts, finished = {}, {}

        def finish(m, done):
            piece = combine(here, row_of(gate_mod, m), after(parts[m], done), planes)
            finished[m] = along(piece, m) if m else piece
            return piece

        waiting = []
        for n, m in enumerate([0] + order[:-1]):
            last = out = down_product(here, after([rows_in[h, m] for h in range(2)], last), blocks[m], down_full)
            parts[m] = [out[0]] + [across(out[b], b) for b in range(1, groups)]
            if waiting and n < planes - 0:
                last = finish(waiting.pop(0), last)
            waiting.append(m)
        for m in waiting:
            last = finish(m, last)
        return place(here, [finished[m] for m in range(planes)], groups)

    return shards_of


def solution(mesh):
    groups, owners = mesh.shape["dp"], mesh.shape["expert"]

    def program(tokens, routes, router_weight, shift, scale, gate_mod, gate_weight, up_weight, down_weight):
        rows = P(AXES, None)
        weights = P(None, AXES, None)
        in_specs = (rows, rows, P(), P(), P(), P(), weights, weights, weights)
        planes = owners // CORES
        whole_lanes = gate_weight.shape[1] == LANES * groups * owners
        powers = groups & (groups - 1) == 0 and planes & (planes - 1) == 0 and owners == planes * CORES
        whole = whole_lanes and powers and planes > 2 and groups > 1 and gate_weight.shape[2] % (2 * LANES * groups) == 0
        body = plane_shards(groups, owners) if whole else routed_shards
        step = jax.shard_map(body, mesh=mesh, in_specs=in_specs, out_specs=rows, check_vma=False)
        return step(tokens, routes, router_weight, shift, scale, gate_mod, gate_weight, up_weight, down_weight)

    return program
```

```python
import jax
import jax.numpy as jnp
from jax import lax
from jax.experimental import pallas as pl
from jax.experimental.pallas import tpu as pltpu
from jax.sharding import PartitionSpec as P


PIX = 4096
EPS = 1e-06
AXES = ("dp", "expert")
CORES = 2
LANES = 128
PIECES = 1


def send_back(output):
    return lax.all_to_all(output, "expert", split_axis=0, concat_axis=0, tiled=True)


def routed_shards(
    tokens, routes, router_weight, shift, scale, gate_mod, gate_weight, up_weight, down_weight
):
    tok_dev = tokens.shape[0]
    width = tokens.shape[1]
    experts = router_weight.shape[1]
    n_owner = lax.axis_size("expert")
    local_count = experts // n_owner
    capacity = max(2, 3 * tok_dev // experts)
    first_row = (lax.axis_index("dp") * n_owner + lax.axis_index("expert")) * tok_dev
    image = first_row // PIX
    shift_row = lax.dynamic_slice_in_dim(shift, image, 1, 0)
    scale_row = lax.dynamic_slice_in_dim(scale, image, 1, 0)
    gate_row = lax.dynamic_slice_in_dim(gate_mod, image, 1, 0)
    values = tokens.astype(jnp.float32)
    meansq = jnp.mean(values * values, axis=-1, keepdims=True)
    normed = (values * lax.rsqrt(meansq + EPS) * (1.0 + scale_row) + shift_row).astype(jnp.bfloat16)
    logits = jnp.dot(normed, router_weight, preferred_element_type=jnp.float32)
    onehot = routes[:, :, None] == jnp.arange(experts, dtype=jnp.int32)[None, None, :]
    chosen = jnp.sum(jnp.where(onehot, logits[:, None, :], 0.0), axis=-1)
    score = jax.nn.sigmoid(chosen)
    flat = routes.reshape(-1)
    hot = (flat[:, None] == jnp.arange(experts, dtype=jnp.int32)[None, :]).astype(jnp.int32)
    rank = jnp.cumsum(hot, axis=0) - hot
    slot = jnp.sum(rank * hot, axis=-1)
    position = flat * capacity + slot
    source = (
        jnp.zeros((experts * capacity,), jnp.int32)
        .at[position]
        .set(jnp.arange(2 * tok_dev, dtype=jnp.int32) // 2)
    )
    filled = jnp.zeros((experts * capacity,), jnp.bool_).at[position].set(True)
    outgoing = jnp.where(filled[:, None], normed[source], jnp.zeros((), jnp.bfloat16)).reshape(
        experts, capacity, width
    )
    quarter_gate, quarter_up, quarter_down = (
        lax.all_to_all(gate_weight, "expert", split_axis=0, concat_axis=1, tiled=True),
        lax.all_to_all(up_weight, "expert", split_axis=0, concat_axis=1, tiled=True),
        lax.all_to_all(down_weight, "expert", split_axis=0, concat_axis=1, tiled=True),
    )
    w_gate, w_up, w_down = (
        lax.all_gather(quarter_gate, "dp", axis=1, tiled=True),
        lax.all_gather(quarter_up, "dp", axis=1, tiled=True),
        lax.all_gather(quarter_down, "dp", axis=1, tiled=True),
    )
    received = lax.all_to_all(outgoing, "expert", split_axis=0, concat_axis=0, tiled=True)
    slots = received.shape[1]
    grid = received.reshape(n_owner, local_count, slots, width)
    gate = jnp.einsum("nxcd,xdf->nxcf", grid, w_gate, preferred_element_type=jnp.float32)
    upper = jnp.einsum("nxcd,xdf->nxcf", grid, w_up, preferred_element_type=jnp.float32)
    hidden = (jax.nn.silu(gate) * upper).astype(jnp.bfloat16)
    output = jnp.einsum(
        "nxcf,xdf->nxcd", hidden, w_down, preferred_element_type=jnp.float32
    ).astype(jnp.bfloat16)
    output = output.reshape(n_owner * local_count, slots, width)
    incoming = send_back(output)
    picked = (
        incoming.reshape(experts * capacity, width)[position]
        .astype(jnp.float32)
        .reshape(tok_dev, 2, width)
    )
    branch = jnp.sum(score[:, :, None] * picked, axis=1)
    return (gate_row * branch).astype(jnp.bfloat16)


def prep_kernel(here, tok_ref, routes_ref, router_ref, shift_ref, scale_ref, *refs):
    outs, norm_ref = refs[:-1], refs[-1]
    z, c = here[1], here[2]
    planes = len(outs)
    tokens, width = tok_ref.shape
    quarter = width // planes
    experts = router_ref.shape[0]
    values = tok_ref[...].astype(jnp.float32)
    meansq = jnp.mean(values * values, axis=-1, keepdims=True)
    normed = values * lax.rsqrt(meansq + EPS) * (1.0 + scale_ref[...]) + shift_ref[...]
    normed = normed.astype(jnp.bfloat16)
    norm_ref[...] = normed
    logits = lax.dot_general(
        normed, router_ref[...], (((1,), (1,)), ((), ())), preferred_element_type=jnp.float32
    )
    ids = lax.broadcasted_iota(jnp.int32, (tokens, experts), 1)
    lane = lax.broadcasted_iota(jnp.int32, (tokens, LANES), 1)
    info = jnp.zeros((tokens, LANES), jnp.float32)
    for k in range(2):
        expert = routes_ref[:, k : k + 1]
        chosen = jnp.sum(jnp.where(ids == expert, logits, 0.0), axis=-1, keepdims=True)
        score = jax.nn.sigmoid(chosen)
        coarse = score.astype(jnp.bfloat16).astype(jnp.float32)
        info = jnp.where(lane == k, expert.astype(jnp.float32), info)
        info = jnp.where(lane == 2 + 2 * k, coarse, info)
        info = jnp.where(lane == 3 + 2 * k, score - coarse, info)
    info = info.astype(jnp.bfloat16)
    rows = LANES
    groups = quarter // (CORES * rows)
    for m, out in enumerate(outs):
        for side in range(CORES):
            for b in range(groups):
                start = ((b * planes + (z ^ m)) * CORES + (c ^ side)) * rows
                at = (side * groups + b) * rows
                out[:, at : at + rows] = norm_ref[:, pl.ds(pl.multiple_of(start, LANES), rows)]
        out[:, quarter:] = info


def prep(here, tokens, routes, router, shift_row, scale_row, planes):
    rows, width = tokens.shape
    block = jax.ShapeDtypeStruct((rows, width // planes + LANES), jnp.bfloat16)
    vmem = pl.BlockSpec(memory_space=pltpu.VMEM)
    return pl.pallas_call(
        prep_kernel,
        in_specs=[pl.BlockSpec(memory_space=pltpu.SMEM)] + [vmem] * 5,
        out_specs=[vmem] * planes,
        out_shape=[block] * planes,
        scratch_shapes=[pltpu.VMEM((rows, width), jnp.bfloat16)],
        name="prep",
    )(here, tokens, routes, router, shift_row, scale_row)


def product_kernel(groups, here, *refs):
    blocks, (first, second), outs, x_ref = refs[:groups], refs[groups : groups + 2], refs[groups + 2 : -1], refs[-1]
    experts, hid = first.shape[1], first.shape[-1]
    each = groups // len(outs)
    tile = blocks[0].shape[0]
    depth = x_ref.shape[1]
    half = depth // CORES
    for i, block in enumerate(blocks):
        at = slice(i * tile, (i + 1) * tile)
        for side in range(CORES):
            for m in range(groups):
                start = pl.multiple_of((side * groups + (here[0] ^ m)) * LANES, LANES)
                to = (side * groups + m) * LANES
                x_ref[at, to : to + LANES] = block[:, pl.ds(start, LANES)]
    routes = [[block[:, depth + k : depth + k + 1].astype(jnp.float32) for k in range(2)] for block in blocks]

    def expert(e, carry):
        mine = e.astype(jnp.float32)
        for part in range(2):
            to = slice(part * hid // 2, (part + 1) * hid // 2)
            weight = jnp.concatenate(
                [ref[:, e, :, to].reshape(half, hid // 2) for ref in (first, second)], axis=0
            )
            product = jnp.dot(x_ref[...], weight, preferred_element_type=jnp.float32)
            for i in range(groups):
                at, out_ref = slice(i % each * tile, (i % each + 1) * tile), outs[i // each]
                for k in range(2):
                    to = slice((2 * k + part) * hid // 2, (2 * k + part + 1) * hid // 2)
                    kept = out_ref[at, to].astype(jnp.float32)
                    value = product[i * tile : (i + 1) * tile]
                    out_ref[at, to] = jnp.where(routes[i][k] == mine, value, kept).astype(jnp.bfloat16)
        return carry

    lax.fori_loop(0, experts, expert, 0, unroll=2)


def expert_product(here, blocks, weights):
    groups, experts, _, hid = weights[0].shape
    tile, lanes = blocks[0].shape
    tokens = groups * tile
    depth = lanes - LANES
    vmem = pl.BlockSpec(memory_space=pltpu.VMEM)
    return pl.pallas_call(
        lambda *refs: product_kernel(groups, *refs),
        in_specs=[pl.BlockSpec(memory_space=pltpu.SMEM)] + [vmem] * (groups + 2),
        out_specs=[vmem] * PIECES,
        out_shape=[jax.ShapeDtypeStruct((tokens // PIECES, 2 * hid), jnp.bfloat16)] * PIECES,
        scratch_shapes=[pltpu.VMEM((tokens, depth), jnp.bfloat16)],
        cost_estimate=pl.CostEstimate(
            flops=experts * 2 * tokens * depth * hid, transcendentals=0, bytes_accessed=4 * weights[0].size
        ),
        compiler_params=pltpu.CompilerParams(vmem_limit_bytes=24 * 2**20),
        name="product",
    )(here, *blocks, *weights)


def hidden_kernel(groups, count, *refs):
    pieces, blocks, out_ref = refs[: count * PIECES], refs[count * PIECES : -1], refs[-1]
    each = groups // PIECES
    hid = out_ref.shape[1] // 2
    tile, lanes = blocks[0].shape
    depth = lanes - LANES
    for i, block in enumerate(blocks):
        at = slice(i % each * tile, (i % each + 1) * tile)
        parts = pieces[i // each :: PIECES]
        for k in range(2):
            score = [block[:, depth + 2 + 2 * k + n : depth + 3 + 2 * k + n].astype(jnp.float32) for n in range(2)]
            sums = []
            for part in range(2):
                to = slice((2 * k + part) * hid, (2 * k + part + 1) * hid)
                total = parts[0][at, to].astype(jnp.float32)
                for other in parts[1:]:
                    total = total + other[at, to].astype(jnp.float32)
                sums.append(total)
            value = sums[0] / (1.0 + jnp.exp(-sums[0])) * sums[1] * (score[0] + score[1])
            out_ref[i * tile : (i + 1) * tile, k * hid : (k + 1) * hid] = value.astype(jnp.bfloat16)


def hidden_rows(parts, blocks):
    groups = len(blocks)
    tokens, columns = parts[0][0].shape[0] * PIECES, parts[0][0].shape[1]
    flat = [piece for part in parts for piece in part]
    vmem = pl.BlockSpec(memory_space=pltpu.VMEM)
    return pl.pallas_call(
        lambda *refs: hidden_kernel(groups, len(parts), *refs),
        in_specs=[vmem] * (len(flat) + groups),
        out_specs=vmem,
        out_shape=jax.ShapeDtypeStruct((tokens, columns // 2), jnp.bfloat16),
        cost_estimate=pl.CostEstimate(flops=10**9, transcendentals=0, bytes_accessed=4 * tokens * columns),
        name="hidden",
    )(*flat, *blocks)


def down_kernel(groups, experts, halves, here, *refs):
    hiddens, blocks, refs = refs[:halves], refs[halves : halves + groups], refs[halves + groups :]
    down_a, down_b, outs, wide_ref = refs[0], refs[1], refs[2 : 2 + groups], refs[-1]
    part = hiddens[0].shape[1] // 2
    hid = part * halves
    tile, lanes = blocks[0].shape
    depth = lanes - LANES
    pair = 2 if groups % 2 == 0 else 1
    zero = jnp.zeros((), jnp.float32)
    for i, block in enumerate(blocks):
        at = slice(i * tile, (i + 1) * tile)
        routes = [block[:, depth + k : depth + k + 1].astype(jnp.float32) for k in range(2)]
        for h, ref in enumerate(hiddens):
            rows = [ref[at, k * part : (k + 1) * part].astype(jnp.float32) for k in range(2)]
            for e in range(experts):
                value = jnp.where(routes[0] == float(e), rows[0], zero)
                value = jnp.where(routes[1] == float(e), rows[1], value)
                to = e * hid + h * part
                wide_ref[at, to : to + part] = value.astype(jnp.bfloat16)
    for side, ref in enumerate((down_a, down_b)):
        for j in range(0, groups, pair):
            weight = jnp.concatenate(
                [jnp.concatenate([ref[j + p, e] for p in range(pair)], axis=0) for e in range(experts)], axis=1
            )
            product = lax.dot_general(
                wide_ref[...], weight, (((1,), (1,)), ((), ())), preferred_element_type=jnp.float32
            ).astype(jnp.bfloat16)
            for p in range(pair):
                start = pl.multiple_of((side * groups + (here[0] ^ (j + p))) * LANES, LANES)
                for i, out in enumerate(outs):
                    out[:, pl.ds(start, LANES)] = product[i * tile : (i + 1) * tile, p * LANES : (p + 1) * LANES]


def down_product(here, hiddens, blocks, down):
    groups, experts, _, hid = down[0].shape
    tile, lanes = blocks[0].shape
    tokens = groups * tile
    width = lanes - LANES
    vmem = pl.BlockSpec(memory_space=pltpu.VMEM)
    return pl.pallas_call(
        lambda *refs: down_kernel(groups, experts, len(hiddens), *refs),
        in_specs=[pl.BlockSpec(memory_space=pltpu.SMEM)] + [vmem] * (len(hiddens) + groups + 2),
        out_specs=[vmem] * groups,
        out_shape=[jax.ShapeDtypeStruct((tile, width), jnp.bfloat16)] * groups,
        scratch_shapes=[pltpu.VMEM((tokens, experts * hid), jnp.bfloat16)],
        cost_estimate=pl.CostEstimate(
            flops=experts * 2 * tokens * width * hid, transcendentals=0, bytes_accessed=2 * down[0].size * 2
        ),
        compiler_params=pltpu.CompilerParams(vmem_limit_bytes=24 * 2**20),
        name="down",
    )(here, *hiddens, *blocks, *down)


def combine_kernel(groups, planes, here, gate_ref, *refs):
    parts, out_ref = refs[:-1], refs[-1]
    z, c = here[1], here[2]
    for side in range(CORES):
        for b in range(groups):
            to = slice((side * groups + b) * LANES, (side * groups + b + 1) * LANES)
            total = parts[0][:, to].astype(jnp.float32)
            for part in parts[1:]:
                total = total + part[:, to].astype(jnp.float32)
            start = pl.multiple_of(((b * planes + z) * CORES + (c ^ side)) * LANES, LANES)
            out_ref[:, to] = (total * gate_ref[:, pl.ds(start, LANES)]).astype(jnp.bfloat16)


def combine(here, gate_row, parts, planes):
    vmem = pl.BlockSpec(memory_space=pltpu.VMEM)
    return pl.pallas_call(
        lambda *refs: combine_kernel(len(parts), planes, *refs),
        in_specs=[pl.BlockSpec(memory_space=pltpu.SMEM)] + [vmem] * (1 + len(parts)),
        out_specs=vmem,
        out_shape=jax.ShapeDtypeStruct(parts[0].shape, jnp.bfloat16),
        name="combine",
    )(here, gate_row, *parts)


def place_kernel(groups, here, *refs):
    pieces, out_ref = refs[:-1], refs[-1]
    planes = len(pieces)
    z, c = here[1], here[2]
    for m, piece in enumerate(pieces):
        for side in range(CORES):
            for b in range(groups):
                start = pl.multiple_of(((b * planes + (z ^ m)) * CORES + (c ^ side)) * LANES, LANES)
                at = (side * groups + b) * LANES
                out_ref[:, pl.ds(start, LANES)] = piece[:, at : at + LANES]


def place(here, pieces, groups):
    tokens, quarter = pieces[0].shape
    vmem = pl.BlockSpec(memory_space=pltpu.VMEM)
    return pl.pallas_call(
        lambda *refs: place_kernel(groups, *refs),
        in_specs=[pl.BlockSpec(memory_space=pltpu.SMEM)] + [vmem] * len(pieces),
        out_specs=vmem,
        out_shape=jax.ShapeDtypeStruct((tokens, quarter * len(pieces)), jnp.bfloat16),
        name="place",
    )(here, *pieces)


def plane_shards(groups, owners):
    planes = owners // CORES

    def flat(g, z, c):
        return (g * planes + z) * CORES + c

    def permute(value, move):
        pairs = []
        for g in range(groups):
            for z in range(planes):
                for c in range(CORES):
                    to = move(g, z, c)
                    if to is not None:
                        pairs.append((flat(g, z, c), flat(*to)))
        return lax.ppermute(value, AXES, pairs)

    def across(value, m):
        return permute(value, lambda g, z, c: (g ^ m, z, c))

    def along(value, m):
        return permute(value, lambda g, z, c: (g, z ^ m, c))

    def swap(value):
        return permute(value, lambda g, z, c: (g, z, c ^ 1))

    def upward(value, senders):
        return permute(value, lambda g, z, c: (g, z + 1, c) if z in senders else None)

    def downward(value, senders):
        return permute(value, lambda g, z, c: (g, z - 1, c) if z in senders else None)

    def after(value, other):
        return lax.optimization_barrier((value, other))[0]

    def add(first, second):
        return (first.astype(jnp.float32) + second.astype(jnp.float32)).astype(jnp.bfloat16)

    def shards_of(tokens, routes, router_weight, shift, scale, gate_mod, gate_weight, up_weight, down_weight):
        tok_dev = tokens.shape[0]
        hid = gate_weight.shape[2] // groups
        g = lax.axis_index("dp")
        owner = lax.axis_index("expert")
        z, c = owner // CORES, owner % CORES
        here = jnp.stack([g, z, c]).astype(jnp.int32)

        def among(names):
            found = jnp.zeros((), jnp.bool_)
            for plane in names:
                found = found | (z == plane)
            return found

        def pick(slots, choice):
            names = sorted(set(choice.values()))
            value = slots[names[0]]
            for name in names[1:]:
                value = jnp.where(among([p for p, slot in choice.items() if slot == name]), slots[name], value)
            return value

        def row_of(table, m):
            image = flat(g, z ^ m, c) * tok_dev // PIX
            return lax.dynamic_slice_in_dim(table, image, 1, 0)

        def share(*weights, columns, start):
            def part(m):
                pieces = [lax.dynamic_slice_in_dim(w, (g ^ m) * hid + start, columns, 2) for w in weights]
                return jnp.concatenate(pieces, axis=2) if len(pieces) > 1 else pieces[0]

            return [part(m) for m in range(groups)]

        def send(parts):
            return parts[:1] + [across(parts[m], m) for m in range(1, groups)]

        far = planes - 1
        order = list(range(far, -1, -1))

        parts0 = send(share(gate_weight, up_weight, columns=hid, start=0))
        split = prep(here, tokens, routes, router_weight.T, row_of(shift, 0), row_of(scale, 0), planes)
        sent = {0: split[0]}
        for m in order[:-1]:
            sent[m] = along(split[m], m)
        cut2 = share(after(down_weight, split), columns=hid, start=0)
        blocks = {}
        for m in order:
            blocks[m] = [sent[m]] + [across(sent[m], b) for b in range(1, groups)]
        parts2 = send(cut2)

        def stack(parts, done):
            full = jnp.stack(after(parts, done))
            return full, (full, swap(full))

        def multiply(m, weights, done):
            return expert_product(here, after(blocks[m], done), weights)

        def moved(s, partial, arrived, done):
            climb = {p: p ^ (planes - s + p) for p in range(0, s)}
            sink = {p: p ^ (s - planes + p) for p in range(planes - s, planes)}
            news = []
            for r in range(PIECES):
                mine = {m: pieces[r] for m, pieces in partial.items()}
                below, above = after(arrived[r], done) if arrived is not None else (None, None)
                if set(climb) & set(sink):
                    rising, falling = pick(mine, climb), pick(mine, sink)
                    if below is not None:
                        rising, falling = add(rising, below), add(falling, above)
                else:
                    rising = pick(mine, {**climb, **sink})
                    if below is not None:
                        rising = add(rising, jnp.where(among(climb), below, above))
                    falling = rising
                done = (rising, falling)
                news.append((upward(rising, set(climb)), downward(falling, set(sink))))
            return news, done

        last, weights = stack(parts0, cut2)
        partial = {far: multiply(far, weights, last)}
        sums, _ = moved(1, {m: partial[far] for m in order}, None, None)
        last = partial[far]
        for m in order[1:-1]:
            last = partial[m] = multiply(m, weights, last)
        whole = {m: partial.get(m, last) for m in order}
        for s in range(2, far):
            sums, last = moved(s, whole, sums, last)
        last = partial[0] = multiply(0, weights, last)
        last, down_full = stack(parts2, last)
        if far > 1:
            sums, last = moved(far, partial, sums, last)
        arrived = after(sums, last)
        belows, aboves = [one[0] for one in arrived], [one[1] for one in arrived]
        hidden = hidden_rows([partial[0], belows, aboves], blocks[0])
        last = hidden
        rows_in = {0: hidden}
        for m in order[:-1]:
            rows_in[m] = along(hidden, m)

        parts, finished = {}, {}

        def finish(m, done):
            piece = combine(here, row_of(gate_mod, m), after(parts[m], done), planes)
            finished[m] = along(piece, m) if m else piece
            return piece

        waiting = []
        for m in range(planes):
            last = out = down_product(here, after([rows_in[m]], last), blocks[m], down_full)
            parts[m] = [out[0]] + [across(out[b], b) for b in range(1, groups)]
            if waiting:
                last = finish(waiting.pop(0), last)
            waiting.append(m)
        for m in waiting:
            last = finish(m, last)
        return place(here, [finished[m] for m in range(planes)], groups)

    return shards_of


def solution(mesh):
    groups, owners = mesh.shape["dp"], mesh.shape["expert"]

    def program(tokens, routes, router_weight, shift, scale, gate_mod, gate_weight, up_weight, down_weight):
        rows = P(AXES, None)
        weights = P(None, AXES, None)
        in_specs = (rows, rows, P(), P(), P(), P(), weights, weights, weights)
        planes = owners // CORES
        whole_lanes = gate_weight.shape[1] == LANES * groups * owners
        powers = groups & (groups - 1) == 0 and planes & (planes - 1) == 0 and owners == planes * CORES
        whole = whole_lanes and powers and planes > 2 and groups > 1 and gate_weight.shape[2] % (2 * LANES * groups) == 0
        body = plane_shards(groups, owners) if whole else routed_shards
        step = jax.shard_map(body, mesh=mesh, in_specs=in_specs, out_specs=rows, check_vma=False)
        return step(tokens, routes, router_weight, shift, scale, gate_mod, gate_weight, up_weight, down_weight)

    return program
```

```python
import jax
import jax.numpy as jnp
from jax import lax
from jax.experimental import pallas as pl
from jax.experimental.pallas import tpu as pltpu
from jax.sharding import PartitionSpec as P


PIX = 4096
EPS = 1e-06
AXES = ("dp", "expert")
CORES = 2
LANES = 128
PIECES = 1


def send_back(output):
    return lax.all_to_all(output, "expert", split_axis=0, concat_axis=0, tiled=True)


def routed_shards(
    tokens, routes, router_weight, shift, scale, gate_mod, gate_weight, up_weight, down_weight
):
    tok_dev = tokens.shape[0]
    width = tokens.shape[1]
    experts = router_weight.shape[1]
    n_owner = lax.axis_size("expert")
    local_count = experts // n_owner
    capacity = max(2, 3 * tok_dev // experts)
    first_row = (lax.axis_index("dp") * n_owner + lax.axis_index("expert")) * tok_dev
    image = first_row // PIX
    shift_row = lax.dynamic_slice_in_dim(shift, image, 1, 0)
    scale_row = lax.dynamic_slice_in_dim(scale, image, 1, 0)
    gate_row = lax.dynamic_slice_in_dim(gate_mod, image, 1, 0)
    values = tokens.astype(jnp.float32)
    meansq = jnp.mean(values * values, axis=-1, keepdims=True)
    normed = (values * lax.rsqrt(meansq + EPS) * (1.0 + scale_row) + shift_row).astype(jnp.bfloat16)
    logits = jnp.dot(normed, router_weight, preferred_element_type=jnp.float32)
    onehot = routes[:, :, None] == jnp.arange(experts, dtype=jnp.int32)[None, None, :]
    chosen = jnp.sum(jnp.where(onehot, logits[:, None, :], 0.0), axis=-1)
    score = jax.nn.sigmoid(chosen)
    flat = routes.reshape(-1)
    hot = (flat[:, None] == jnp.arange(experts, dtype=jnp.int32)[None, :]).astype(jnp.int32)
    rank = jnp.cumsum(hot, axis=0) - hot
    slot = jnp.sum(rank * hot, axis=-1)
    position = flat * capacity + slot
    source = (
        jnp.zeros((experts * capacity,), jnp.int32)
        .at[position]
        .set(jnp.arange(2 * tok_dev, dtype=jnp.int32) // 2)
    )
    filled = jnp.zeros((experts * capacity,), jnp.bool_).at[position].set(True)
    outgoing = jnp.where(filled[:, None], normed[source], jnp.zeros((), jnp.bfloat16)).reshape(
        experts, capacity, width
    )
    quarter_gate, quarter_up, quarter_down = (
        lax.all_to_all(gate_weight, "expert", split_axis=0, concat_axis=1, tiled=True),
        lax.all_to_all(up_weight, "expert", split_axis=0, concat_axis=1, tiled=True),
        lax.all_to_all(down_weight, "expert", split_axis=0, concat_axis=1, tiled=True),
    )
    w_gate, w_up, w_down = (
        lax.all_gather(quarter_gate, "dp", axis=1, tiled=True),
        lax.all_gather(quarter_up, "dp", axis=1, tiled=True),
        lax.all_gather(quarter_down, "dp", axis=1, tiled=True),
    )
    received = lax.all_to_all(outgoing, "expert", split_axis=0, concat_axis=0, tiled=True)
    slots = received.shape[1]
    grid = received.reshape(n_owner, local_count, slots, width)
    gate = jnp.einsum("nxcd,xdf->nxcf", grid, w_gate, preferred_element_type=jnp.float32)
    upper = jnp.einsum("nxcd,xdf->nxcf", grid, w_up, preferred_element_type=jnp.float32)
    hidden = (jax.nn.silu(gate) * upper).astype(jnp.bfloat16)
    output = jnp.einsum(
        "nxcf,xdf->nxcd", hidden, w_down, preferred_element_type=jnp.float32
    ).astype(jnp.bfloat16)
    output = output.reshape(n_owner * local_count, slots, width)
    incoming = send_back(output)
    picked = (
        incoming.reshape(experts * capacity, width)[position]
        .astype(jnp.float32)
        .reshape(tok_dev, 2, width)
    )
    branch = jnp.sum(score[:, :, None] * picked, axis=1)
    return (gate_row * branch).astype(jnp.bfloat16)


def prep_kernel(here, tok_ref, routes_ref, router_ref, shift_ref, scale_ref, *refs):
    outs, norm_ref = refs[:-1], refs[-1]
    z, c = here[1], here[2]
    planes = len(outs)
    tokens, width = tok_ref.shape
    quarter = width // planes
    experts = router_ref.shape[0]
    values = tok_ref[...].astype(jnp.float32)
    meansq = jnp.mean(values * values, axis=-1, keepdims=True)
    normed = values * lax.rsqrt(meansq + EPS) * (1.0 + scale_ref[...]) + shift_ref[...]
    normed = normed.astype(jnp.bfloat16)
    norm_ref[...] = normed
    logits = lax.dot_general(
        normed, router_ref[...], (((1,), (1,)), ((), ())), preferred_element_type=jnp.float32
    )
    ids = lax.broadcasted_iota(jnp.int32, (tokens, experts), 1)
    lane = lax.broadcasted_iota(jnp.int32, (tokens, LANES), 1)
    info = jnp.zeros((tokens, LANES), jnp.float32)
    for k in range(2):
        expert = routes_ref[:, k : k + 1]
        chosen = jnp.sum(jnp.where(ids == expert, logits, 0.0), axis=-1, keepdims=True)
        score = jax.nn.sigmoid(chosen)
        coarse = score.astype(jnp.bfloat16).astype(jnp.float32)
        info = jnp.where(lane == k, expert.astype(jnp.float32), info)
        info = jnp.where(lane == 2 + 2 * k, coarse, info)
        info = jnp.where(lane == 3 + 2 * k, score - coarse, info)
    info = info.astype(jnp.bfloat16)
    rows = LANES
    groups = quarter // (CORES * rows)
    for m, out in enumerate(outs):
        for side in range(CORES):
            for b in range(groups):
                start = ((b * planes + (z ^ m)) * CORES + (c ^ side)) * rows
                at = (side * groups + b) * rows
                out[:, at : at + rows] = norm_ref[:, pl.ds(pl.multiple_of(start, LANES), rows)]
        out[:, quarter:] = info


def prep(here, tokens, routes, router, shift_row, scale_row, planes):
    rows, width = tokens.shape
    block = jax.ShapeDtypeStruct((rows, width // planes + LANES), jnp.bfloat16)
    vmem = pl.BlockSpec(memory_space=pltpu.VMEM)
    return pl.pallas_call(
        prep_kernel,
        in_specs=[pl.BlockSpec(memory_space=pltpu.SMEM)] + [vmem] * 5,
        out_specs=[vmem] * planes,
        out_shape=[block] * planes,
        scratch_shapes=[pltpu.VMEM((rows, width), jnp.bfloat16)],
        name="prep",
    )(here, tokens, routes, router, shift_row, scale_row)


def product_kernel(groups, here, *refs):
    blocks, (first, second), outs = refs[:groups], refs[groups : groups + 2], refs[groups + 2 : -2]
    info_ref, x_ref = refs[-2:]
    experts, hid = first.shape[1], first.shape[-1]
    each = groups // len(outs)
    tile = blocks[0].shape[0]
    depth = x_ref.shape[1]
    half = depth // CORES
    for i, block in enumerate(blocks):
        at = slice(i * tile, (i + 1) * tile)
        for side in range(CORES):
            for m in range(groups):
                start = pl.multiple_of((side * groups + (here[0] ^ m)) * LANES, LANES)
                to = (side * groups + m) * LANES
                x_ref[at, to : to + LANES] = block[:, pl.ds(start, LANES)]
        info_ref[at, :] = block[:, depth:]
    routes = [[block[:, depth + k : depth + k + 1].astype(jnp.float32) for k in range(2)] for block in blocks]

    def expert(e, carry):
        mine = e.astype(jnp.float32)
        for part in range(2):
            to = slice(part * hid // 2, (part + 1) * hid // 2)
            weight = jnp.concatenate(
                [ref[:, e, :, to].reshape(half, hid // 2) for ref in (first, second)], axis=0
            )
            product = jnp.dot(x_ref[...], weight, preferred_element_type=jnp.float32)
            for i in range(groups):
                at, out_ref = slice(i % each * tile, (i % each + 1) * tile), outs[i // each]
                for k in range(2):
                    to = slice((2 * k + part) * hid // 2, (2 * k + part + 1) * hid // 2)
                    kept = out_ref[at, to].astype(jnp.float32)
                    value = product[i * tile : (i + 1) * tile]
                    out_ref[at, to] = jnp.where(routes[i][k] == mine, value, kept).astype(jnp.bfloat16)
        return carry

    lax.fori_loop(0, experts, expert, 0, unroll=2)


def expert_product(here, blocks, weights):
    groups, experts, _, hid = weights[0].shape
    tile, lanes = blocks[0].shape
    tokens = groups * tile
    depth = lanes - LANES
    vmem = pl.BlockSpec(memory_space=pltpu.VMEM)
    return pl.pallas_call(
        lambda *refs: product_kernel(groups, *refs),
        in_specs=[pl.BlockSpec(memory_space=pltpu.SMEM)] + [vmem] * (groups + 2),
        out_specs=[vmem] * (PIECES + 1),
        out_shape=[jax.ShapeDtypeStruct((tokens // PIECES, 2 * hid), jnp.bfloat16)] * PIECES
        + [jax.ShapeDtypeStruct((tokens, LANES), jnp.bfloat16)],
        scratch_shapes=[pltpu.VMEM((tokens, depth), jnp.bfloat16)],
        cost_estimate=pl.CostEstimate(
            flops=experts * 2 * tokens * depth * hid, transcendentals=0, bytes_accessed=4 * weights[0].size
        ),
        compiler_params=pltpu.CompilerParams(vmem_limit_bytes=24 * 2**20),
        name="product",
    )(here, *blocks, *weights)


def hidden_kernel(groups, count, *refs):
    pieces, info_ref, out_ref = refs[: count * PIECES], refs[-2], refs[-1]
    each = groups // PIECES
    hid = out_ref.shape[1] // 2
    tile = info_ref.shape[0] // groups
    for i in range(groups):
        at = slice(i % each * tile, (i % each + 1) * tile)
        info = info_ref[i * tile : (i + 1) * tile, :].astype(jnp.float32)
        parts = pieces[i // each :: PIECES]
        for k in range(2):
            score = [info[:, 2 + 2 * k + n : 3 + 2 * k + n] for n in range(2)]
            sums = []
            for part in range(2):
                to = slice((2 * k + part) * hid, (2 * k + part + 1) * hid)
                total = parts[0][at, to].astype(jnp.float32)
                for other in parts[1:]:
                    total = total + other[at, to].astype(jnp.float32)
                sums.append(total)
            value = sums[0] / (1.0 + jnp.exp(-sums[0])) * sums[1] * (score[0] + score[1])
            out_ref[i * tile : (i + 1) * tile, k * hid : (k + 1) * hid] = value.astype(jnp.bfloat16)


def hidden_rows(parts, info, groups):
    tokens, columns = parts[0][0].shape[0] * PIECES, parts[0][0].shape[1]
    flat = [piece for part in parts for piece in part]
    vmem = pl.BlockSpec(memory_space=pltpu.VMEM)
    return pl.pallas_call(
        lambda *refs: hidden_kernel(groups, len(parts), *refs),
        in_specs=[vmem] * (len(flat) + 1),
        out_specs=vmem,
        out_shape=jax.ShapeDtypeStruct((tokens, columns // 2), jnp.bfloat16),
        cost_estimate=pl.CostEstimate(flops=10**9, transcendentals=0, bytes_accessed=4 * tokens * columns),
        name="hidden",
    )(*flat, info)


def down_kernel(groups, experts, halves, here, *refs):
    hiddens, info_ref, refs = refs[:halves], refs[halves], refs[halves + 1 :]
    down_a, down_b, outs, wide_ref = refs[0], refs[1], refs[2 : 2 + groups], refs[-1]
    part = hiddens[0].shape[1] // 2
    hid = part * halves
    tile = info_ref.shape[0] // groups
    pair = 2 if groups % 2 == 0 else 1
    zero = jnp.zeros((), jnp.float32)
    for i in range(groups):
        at = slice(i * tile, (i + 1) * tile)
        routes = [info_ref[at, k : k + 1].astype(jnp.float32) for k in range(2)]
        for h, ref in enumerate(hiddens):
            rows = [ref[at, k * part : (k + 1) * part].astype(jnp.float32) for k in range(2)]
            for e in range(experts):
                value = jnp.where(routes[0] == float(e), rows[0], zero)
                value = jnp.where(routes[1] == float(e), rows[1], value)
                to = e * hid + h * part
                wide_ref[at, to : to + part] = value.astype(jnp.bfloat16)
    for side, ref in enumerate((down_a, down_b)):
        for j in range(0, groups, pair):
            weight = jnp.concatenate(
                [jnp.concatenate([ref[j + p, e] for p in range(pair)], axis=0) for e in range(experts)], axis=1
            )
            product = lax.dot_general(
                wide_ref[...], weight, (((1,), (1,)), ((), ())), preferred_element_type=jnp.float32
            ).astype(jnp.bfloat16)
            for p in range(pair):
                start = pl.multiple_of((side * groups + (here[0] ^ (j + p))) * LANES, LANES)
                for i, out in enumerate(outs):
                    out[:, pl.ds(start, LANES)] = product[i * tile : (i + 1) * tile, p * LANES : (p + 1) * LANES]


def down_product(here, hiddens, info, down):
    groups, experts, rows, hid = down[0].shape
    tokens = info.shape[0]
    tile = tokens // groups
    width = CORES * groups * rows
    vmem = pl.BlockSpec(memory_space=pltpu.VMEM)
    return pl.pallas_call(
        lambda *refs: down_kernel(groups, experts, len(hiddens), *refs),
        in_specs=[pl.BlockSpec(memory_space=pltpu.SMEM)] + [vmem] * (len(hiddens) + 3),
        out_specs=[vmem] * groups,
        out_shape=[jax.ShapeDtypeStruct((tile, width), jnp.bfloat16)] * groups,
        scratch_shapes=[pltpu.VMEM((tokens, experts * hid), jnp.bfloat16)],
        cost_estimate=pl.CostEstimate(
            flops=experts * 2 * tokens * width * hid, transcendentals=0, bytes_accessed=2 * down[0].size * 2
        ),
        compiler_params=pltpu.CompilerParams(vmem_limit_bytes=24 * 2**20),
        name="down",
    )(here, *hiddens, info, *down)


def combine_kernel(groups, planes, here, gate_ref, *refs):
    parts, out_ref = refs[:-1], refs[-1]
    z, c = here[1], here[2]
    for side in range(CORES):
        for b in range(groups):
            to = slice((side * groups + b) * LANES, (side * groups + b + 1) * LANES)
            total = parts[0][:, to].astype(jnp.float32)
            for part in parts[1:]:
                total = total + part[:, to].astype(jnp.float32)
            start = pl.multiple_of(((b * planes + z) * CORES + (c ^ side)) * LANES, LANES)
            out_ref[:, to] = (total * gate_ref[:, pl.ds(start, LANES)]).astype(jnp.bfloat16)


def combine(here, gate_row, parts, planes):
    vmem = pl.BlockSpec(memory_space=pltpu.VMEM)
    return pl.pallas_call(
        lambda *refs: combine_kernel(len(parts), planes, *refs),
        in_specs=[pl.BlockSpec(memory_space=pltpu.SMEM)] + [vmem] * (1 + len(parts)),
        out_specs=vmem,
        out_shape=jax.ShapeDtypeStruct(parts[0].shape, jnp.bfloat16),
        name="combine",
    )(here, gate_row, *parts)


def place_kernel(groups, here, *refs):
    pieces, out_ref = refs[:-1], refs[-1]
    planes = len(pieces)
    z, c = here[1], here[2]
    for m, piece in enumerate(pieces):
        for side in range(CORES):
            for b in range(groups):
                start = pl.multiple_of(((b * planes + (z ^ m)) * CORES + (c ^ side)) * LANES, LANES)
                at = (side * groups + b) * LANES
                out_ref[:, pl.ds(start, LANES)] = piece[:, at : at + LANES]


def place(here, pieces, groups):
    tokens, quarter = pieces[0].shape
    vmem = pl.BlockSpec(memory_space=pltpu.VMEM)
    return pl.pallas_call(
        lambda *refs: place_kernel(groups, *refs),
        in_specs=[pl.BlockSpec(memory_space=pltpu.SMEM)] + [vmem] * len(pieces),
        out_specs=vmem,
        out_shape=jax.ShapeDtypeStruct((tokens, quarter * len(pieces)), jnp.bfloat16),
        name="place",
    )(here, *pieces)


def plane_shards(groups, owners):
    planes = owners // CORES

    def flat(g, z, c):
        return (g * planes + z) * CORES + c

    def permute(value, move):
        pairs = []
        for g in range(groups):
            for z in range(planes):
                for c in range(CORES):
                    to = move(g, z, c)
                    if to is not None:
                        pairs.append((flat(g, z, c), flat(*to)))
        return lax.ppermute(value, AXES, pairs)

    def across(value, m):
        return permute(value, lambda g, z, c: (g ^ m, z, c))

    def along(value, m):
        return permute(value, lambda g, z, c: (g, z ^ m, c))

    def swap(value):
        return permute(value, lambda g, z, c: (g, z, c ^ 1))

    def upward(value, senders):
        return permute(value, lambda g, z, c: (g, z + 1, c) if z in senders else None)

    def downward(value, senders):
        return permute(value, lambda g, z, c: (g, z - 1, c) if z in senders else None)

    def after(value, other):
        return lax.optimization_barrier((value, other))[0]

    def add(first, second):
        return (first.astype(jnp.float32) + second.astype(jnp.float32)).astype(jnp.bfloat16)

    def shards_of(tokens, routes, router_weight, shift, scale, gate_mod, gate_weight, up_weight, down_weight):
        tok_dev = tokens.shape[0]
        hid = gate_weight.shape[2] // groups
        g = lax.axis_index("dp")
        owner = lax.axis_index("expert")
        z, c = owner // CORES, owner % CORES
        here = jnp.stack([g, z, c]).astype(jnp.int32)

        def among(names):
            found = jnp.zeros((), jnp.bool_)
            for plane in names:
                found = found | (z == plane)
            return found

        def pick(slots, choice):
            names = sorted(set(choice.values()))
            value = slots[names[0]]
            for name in names[1:]:
                value = jnp.where(among([p for p, slot in choice.items() if slot == name]), slots[name], value)
            return value

        def row_of(table, m):
            image = flat(g, z ^ m, c) * tok_dev // PIX
            return lax.dynamic_slice_in_dim(table, image, 1, 0)

        def share(*weights, columns, start):
            def part(m):
                pieces = [lax.dynamic_slice_in_dim(w, (g ^ m) * hid + start, columns, 2) for w in weights]
                return jnp.concatenate(pieces, axis=2) if len(pieces) > 1 else pieces[0]

            return [part(m) for m in range(groups)]

        def send(parts):
            return parts[:1] + [across(parts[m], m) for m in range(1, groups)]

        far = planes - 1
        order = list(range(far, -1, -1))

        parts0 = send(share(gate_weight, up_weight, columns=hid, start=0))
        split = prep(here, tokens, routes, router_weight.T, row_of(shift, 0), row_of(scale, 0), planes)
        sent = {0: split[0]}
        for m in order[:-1]:
            sent[m] = along(split[m], m)
        cut2 = share(after(down_weight, split), columns=hid, start=0)
        blocks = {}
        for m in order:
            blocks[m] = [sent[m]] + [across(sent[m], b) for b in range(1, groups)]
        parts2 = send(cut2)

        def stack(parts, done):
            full = jnp.stack(after(parts, done))
            return full, (full, swap(full))

        infos = {}

        def multiply(m, weights, done):
            *pieces, infos[m] = expert_product(here, after(blocks[m], done), weights)
            return pieces

        def moved(s, partial, arrived, done):
            climb = {p: p ^ (planes - s + p) for p in range(0, s)}
            sink = {p: p ^ (s - planes + p) for p in range(planes - s, planes)}
            news = []
            for r in range(PIECES):
                mine = {m: pieces[r] for m, pieces in partial.items()}
                below = above = None
                if arrived is not None and arrived[r][0] is arrived[r][1]:
                    below = above = after(arrived[r][0], done)
                elif arrived is not None:
                    below, above = after(arrived[r], done)
                if set(climb) & set(sink):
                    rising, falling = pick(mine, climb), pick(mine, sink)
                    if below is not None:
                        rising, falling = add(rising, below), add(falling, above)
                else:
                    rising = pick(mine, {**climb, **sink})
                    if below is not None:
                        rising = add(rising, below if below is above else jnp.where(among(climb), below, above))
                    falling = rising
                done = (rising, falling)
                apart = not {p + 1 for p in climb} & {p - 1 for p in sink} and not set(climb) & set(sink)
                if apart:
                    both = permute(
                        rising,
                        lambda g, z, c: (g, z + 1, c) if z in climb else (g, z - 1, c) if z in sink else None,
                    )
                    news.append((both, both))
                else:
                    news.append((upward(rising, set(climb)), downward(falling, set(sink))))
            return news, done

        last, weights = stack(parts0, cut2)
        partial = {far: multiply(far, weights, last)}
        sums, _ = moved(1, {m: partial[far] for m in order}, None, None)
        last = partial[far]
        for m in order[1:-1]:
            last = partial[m] = multiply(m, weights, last)
        whole = {m: partial.get(m, last) for m in order}
        for s in range(2, far):
            sums, last = moved(s, whole, sums, last)
        last = partial[0] = multiply(0, weights, last)
        last, down_full = stack(parts2, last)
        if far > 1:
            sums, last = moved(far, partial, sums, last)
        arrived = after(sums, last)
        belows, aboves = [one[0] for one in arrived], [one[1] for one in arrived]
        hidden = hidden_rows([partial[0], belows, aboves], infos[0], groups)
        last = hidden
        rows_in = {0: hidden}
        for m in order[:-1]:
            rows_in[m] = along(hidden, m)

        parts, finished = {}, {}

        def finish(m, done):
            piece = combine(here, row_of(gate_mod, m), after(parts[m], done), planes)
            finished[m] = along(piece, m) if m else piece
            return piece

        waiting = []
        for m in range(planes):
            last = out = down_product(here, after([rows_in[m]], last), infos[m], down_full)
            parts[m] = [out[0]] + [across(out[b], b) for b in range(1, groups)]
            if waiting and m == 1:
                last = finish(waiting.pop(0), last)
            waiting.append(m)
        for m in waiting[1:-1] + waiting[:1] + waiting[-1:]:
            last = finish(m, last)
        return place(here, [finished[m] for m in range(planes)], groups)

    return shards_of


def solution(mesh):
    groups, owners = mesh.shape["dp"], mesh.shape["expert"]

    def program(tokens, routes, router_weight, shift, scale, gate_mod, gate_weight, up_weight, down_weight):
        rows = P(AXES, None)
        weights = P(None, AXES, None)
        in_specs = (rows, rows, P(), P(), P(), P(), weights, weights, weights)
        planes = owners // CORES
        whole_lanes = gate_weight.shape[1] == LANES * groups * owners
        powers = groups & (groups - 1) == 0 and planes & (planes - 1) == 0 and owners == planes * CORES
        whole = whole_lanes and powers and planes > 2 and groups > 1 and gate_weight.shape[2] % (2 * LANES * groups) == 0
        body = plane_shards(groups, owners) if whole else routed_shards
        step = jax.shard_map(body, mesh=mesh, in_specs=in_specs, out_specs=rows, check_vma=False)
        return step(tokens, routes, router_weight, shift, scale, gate_mod, gate_weight, up_weight, down_weight)

    return program
```
